256 devices in a mesh: blk: 128 (over z_lo, y, x, core), rep: 2 (over z_hi).
Axes of the slice: x: 4, y: 4, z: 8 (z_hi: 2, z_lo: 4; z = z_hi * 4 + z_lo), core: 2. Of those that a mesh axis runs over, the one named last changes fastest.
Arguments:
- load_coef: bfloat16 [256, 2049, 256], P('blk', None, 'rep'), parts along dimension 2, may hold values from -0.29882812 to 0.29882812
- legendre: bfloat16 [256, 2049, 1024], P('blk'), may hold values from -0.125 to 0.125
- slab_orders: int32 [256], replicated, may hold values from 0 to 1023, as said below
- cycle_rows: int32 [1024], replicated, may hold values from 0 to 1023, each once
Outputs:
- potential: bfloat16 [1024, 128, 4096], P('blk', 'rep'), parts along dimension 1
- energy: float32 [128], P('rep'), parts along dimension 0
The draws below stay inside these ranges and needn't reach their ends.
There are 2 independent parts, one for each index of `rep`. The reference program is written for one: setup_inputs(seed, part) draws one part's arguments, and reference() takes and returns one part's arrays. A program takes and returns all parts, laid end to end along the dimension named above; an argument that names none is the same for every part. Nothing has to cross between parts.
Inputs may be any that keep to these rules, and one draw needn't show every extreme that they name: `slab_orders`: values are distinct and below (2048) / 2. `cycle_rows`: each cycle appears once.
All inputs are finite; a program needn't handle non-finite values.
Results may differ from the reference program's by a relative error of at most 0.0055.
Values may be sent and summed in bfloat16 or wider, within the bound.
A program may use at most 128 MiB of HBM per device.

```python
import math
import jax
import jax.numpy as jnp
from jax import lax

DEGREE = 2047
NLAT = 1024
NLON = 4096
FIELDS = 64
SLAB = 2049
PAIRS = 256


def draw_slab_orders(key, part):
    return jax.random.permutation(key, (DEGREE + 1) // 2)[:PAIRS].astype(jnp.int32)


def levels(key, dims, shards, smallest, top_value):
    loudness = 1.0
    for axis_at, blocks in shards:
        draws = jax.random.uniform(jax.random.fold_in(jax.random.fold_in(key, 6), axis_at), (blocks,), jnp.float32, smallest / len(shards), top_value / len(shards))
        loudness = loudness * jnp.repeat(jnp.exp(draws), dims[axis_at] // blocks).reshape((-1,) + (1,) * (len(dims) - 1 - axis_at))
    return loudness


def scatter_about(key, dims, scale, limit, pieces=(), kind=jnp.bfloat16):
    values = jax.random.normal(key, dims, jnp.float32) * scale
    if len(pieces) > 0:
        values = levels(key, dims, pieces, -0.22, 0.18) * values
    return jnp.clip(values, min=-limit, max=limit).astype(kind)


def setup_inputs(seed: int = 0, part: int = 0) -> dict:
    streams_of = jax.random.split(jax.random.key(seed), 5)
    part_splits = jax.random.split(jax.random.fold_in(streams_of[4], part), 5)
    load_coef = scatter_about(part_splits[0], (PAIRS, SLAB, 2 * FIELDS), 0.05, 0.29882812, ((0, 128),))
    legendre = scatter_about(streams_of[1], (PAIRS, SLAB, NLAT), SLAB ** -0.5, 0.125, ((0, 128),))
    slab_orders = draw_slab_orders(jax.random.fold_in(streams_of[4], 71), part)
    cycle_rows = jax.random.permutation(streams_of[3], NLAT).astype(jnp.int32)
    return {"load_coef": load_coef, "legendre": legendre, "slab_orders": slab_orders, "cycle_rows": cycle_rows}


def basis_table(orders):
    longitude_ids = jnp.arange(NLON, dtype=jnp.int32)
    phase_ids = (orders[:, None] * longitude_ids[None, :]) % NLON
    angles = phase_ids.astype(jnp.float32) * (2.0 * math.pi / NLON)
    factor = jnp.where(orders == 0, 1.0, 2.0).astype(jnp.float32)[:, None]
    return (factor * jnp.cos(angles)).astype(jnp.bfloat16), (-factor * jnp.sin(angles)).astype(jnp.bfloat16)


def reference(load_coef, legendre, slab_orders, cycle_rows):
    slab_rows = DEGREE + 2
    row_ids = jnp.arange(slab_rows, dtype=jnp.int32)

    def synthesize(pair_args):
        pair_coef, pair_table, low_order = pair_args
        in_lower = (row_ids < slab_rows - 1 - low_order)[:, None]
        nothing = jnp.zeros_like(pair_coef)
        stacked = jnp.concatenate([jnp.where(in_lower, pair_coef, nothing), jnp.where(in_lower, nothing, pair_coef)], axis=1)
        return lax.dot_general(stacked, pair_table, (((0,), (0,)), ((), ())), preferred_element_type=jnp.float32).astype(jnp.bfloat16)

    spectra = lax.map(synthesize, (load_coef, legendre, slab_orders))
    spectra = spectra.reshape(PAIRS, 4, FIELDS, NLAT)
    cos_lower, sin_lower = basis_table(slab_orders.astype(jnp.int32))
    cos_upper, sin_upper = basis_table((DEGREE - slab_orders).astype(jnp.int32))
    basis = jnp.stack([cos_lower, sin_lower, cos_upper, sin_upper], axis=1).reshape(PAIRS * 4, NLON)

    def per_field(field_index):
        rows = spectra[:, :, field_index, :].reshape(PAIRS * 4, NLAT)
        wave = lax.dot_general(rows, basis, (((0,), (0,)), ((), ())), preferred_element_type=jnp.float32)
        energy = jnp.sum(wave * wave) / (NLAT * NLON)
        return wave[cycle_rows].astype(jnp.bfloat16), energy

    potential, energy = lax.map(per_field, jnp.arange(FIELDS, dtype=jnp.int32))
    return jnp.transpose(potential, (1, 0, 2)), energy
```

```python
import math

import jax
import jax.numpy as jnp
from jax import lax
from jax.experimental import pallas as pl
from jax.experimental.pallas import tpu as pltpu
from jax.sharding import PartitionSpec as P

BF16 = jnp.bfloat16
F32 = jnp.float32
I32 = jnp.int32
MESH = pl.DeviceIdType.MESH
NLON = 4096
HALF = NLON // 2
DEGREE = 2047
ROWS = 2049
NLAT = 1024
FIELDS = 64
NBLK = 128
PLANE = 32
COLS = 512


def sincos(phase):
    turned = (phase + 512) & 4095
    quadrant = turned >> 10
    theta = ((turned & 1023) - 512).astype(F32) * (2.0 * math.pi / NLON)
    t2 = theta * theta
    s = theta * (1.0 + t2 * (-1.0 / 6 + t2 * (1.0 / 120 + t2 * (-1.0 / 5040 + t2 * (1.0 / 362880)))))
    c = 1.0 + t2 * (-0.5 + t2 * (1.0 / 24 + t2 * (-1.0 / 720 + t2 * (1.0 / 40320))))
    odd = (quadrant & 1) == 1
    cosine = jnp.where(odd, s, c)
    sine = jnp.where(odd, c, s)
    flip_cos = ((quadrant + 1) & 2) == 2
    flip_sin = (quadrant & 2) == 2
    return jnp.where(flip_cos, -cosine, cosine), jnp.where(flip_sin, -sine, sine)


def exchange(
    orders_hbm, cycles_hbm, coef_hbm, leg_hbm,
    even_x, odd_x, basis, energy_ref,
    orders_v, cycles, coef, leg, stacked, spec, onehot, outbox, inbox, wide, order_cols, e_mine, e_plane, e_all,
    small_sems, coef_sem, leg_sem, send_sem, recv_sem, e_sems, ring_sems,
):
    me = lax.axis_index("blk")
    z, y, x, c = me // 32, (me // 8) % 4, (me // 2) % 4, me % 2

    def at(dz, dy, dx, dc):
        return (((z + dz) % 4 * 4 + (y + dy) % 4) * 4 + (x + dx) % 4) * 2 + (c + dc) % 2

    near = [(d, 0, 0, 0) for d in (1, 2, 3)] + [(0, d, 0, 0) for d in (1, 2, 3)]
    near += [(0, 0, d, 0) for d in (1, 2, 3)] + [(0, 0, 0, 1)]

    orders_copy = pltpu.make_async_copy(orders_hbm, orders_v, small_sems.at[0])
    orders_copy.start()
    cycles_copy = pltpu.make_async_copy(cycles_hbm, cycles, small_sems.at[1])
    cycles_copy.start()
    coef_copy = pltpu.make_async_copy(coef_hbm, coef, coef_sem)
    coef_copy.start()
    leg_copies = [pltpu.make_async_copy(leg_hbm.at[:, jt], leg.at[jt], leg_sem.at[jt]) for jt in range(8)]
    for copy in leg_copies:
        copy.start()

    barrier = pltpu.get_barrier_semaphore()

    def signal(sem):
        for offset in near:
            pl.semaphore_signal(sem, inc=1, device_id={"blk": at(*offset)}, device_id_type=MESH)

    signal(barrier)

    orders_copy.wait()
    for h in range(2):
        order_cols[h * 128 : (h + 1) * 128, :] = jnp.broadcast_to(orders_v[h : h + 1, :], (128, 128)).T
    cycles_copy.wait()
    lanes = lax.broadcasted_iota(I32, (128, 128), 1)
    for ib in range(8):
        wanted = jnp.broadcast_to(cycles[ib : ib + 1, :], (128, 128)).T
        for jb in range(8):
            onehot[ib * 128 : (ib + 1) * 128, jb * 128 : (jb + 1) * 128] = jnp.where(
                wanted == lanes + jb * 128, 1.0, 0.0
            ).astype(BF16)

    coef_copy.wait()
    packed = coef[...].reshape(2 * ROWS, 128).T
    column = lax.broadcasted_iota(I32, (1, 2 * ROWS), 1)
    row_id, pair_id = column >> 1, column & 1
    for p in range(2):
        order = order_cols[pl.ds(me * 2 + p, 1), :][:, :1]
        lower = jnp.where(row_id < DEGREE + 1 - order, 1, 0)
        parity_of = jnp.where(pair_id == p, (lower + order + 1) & 1, 2)
        for parity in range(2):
            keep = jnp.where(parity_of == parity, 1.0, 0.0).astype(BF16)
            for part in range(2):
                row = ((p * 2 + part) * 2 + parity) * 64
                stacked[row : row + 64, :] = packed[part * 64 : (part + 1) * 64] * keep

    pl.semaphore_wait(barrier, 10)
    signal(ring_sems.at[0])
    for jp in range(4):
        leg_copies[2 * jp].wait()
        leg_copies[2 * jp + 1].wait()
        table = jnp.concatenate(
            [leg[2 * jp].reshape(2 * ROWS, 128), leg[2 * jp + 1].reshape(2 * ROWS, 128)], axis=1
        )
        spec[:, jp * 256 : (jp + 1) * 256] = jnp.dot(
            stacked[...], table, preferred_element_type=F32
        ).astype(BF16)
        if jp == 2:
            pl.semaphore_wait(ring_sems.at[0], 10)
            signal(ring_sems.at[1])
    outbox[...] = (
        lax.dot_general(onehot[...], spec[...], (((1,), (1,)), ((), ())), preferred_element_type=F32)
        .reshape(NBLK, 8, COLS)
        .astype(BF16)
    )

    def send(dz, dy, dx, dc):
        target = at(dz, dy, dx, dc)
        pltpu.make_async_remote_copy(
            src_ref=outbox.at[target], dst_ref=inbox.at[me], send_sem=send_sem, recv_sem=recv_sem.at[dz],
            device_id={"blk": target}, device_id_type=MESH,
        ).start()

    def send_all(planes, axes, flip):
        count = 3 ** len(axes)

        def one(t, carry):
            offset = [0, 0, 0, flip]
            rest = t
            for axis in axes:
                offset[axis] = rest % 3 + 1
                rest = rest // 3
            for dz in planes:
                send(dz, *offset[1:])
            return carry

        if count == 1:
            one(0, 0)
        else:
            lax.fori_loop(0, count, one, 0)

    across = (2, 1, 3)
    send_all(across, (), 0)
    send_all((2, 1, 3, 0), (2,), 0)
    send_all((2, 1, 3, 0), (1,), 0)
    send_all((2, 1, 3, 0), (), 1)
    for axes, flip in (((1, 2), 0), ((1,), 1), ((2,), 1)):
        send_all((0,), axes, flip)
    pl.semaphore_wait(ring_sems.at[1], 10)
    signal(ring_sems.at[2])
    for axes, flip in (((1, 2), 0), ((1,), 1), ((2,), 1)):
        send_all((2,), axes, flip)
    send_all((0,), (1, 2), 1)
    pl.semaphore_wait(ring_sems.at[2], 10)
    send_all((2,), (1, 2), 1)
    for axes, flip in (((1, 2), 0), ((1,), 1), ((2,), 1), ((1, 2), 1)):
        send_all((1, 3), axes, flip)
    inbox[me] = outbox[me]

    place = me % PLANE
    is_even = lax.broadcasted_iota(I32, (1, 128), 1) < FIELDS
    energy = jnp.zeros((1, 128), F32)
    for p in range(2):
        order = order_cols[pl.ds(me * 2 + p, 1), :]
        has_zero = jnp.where(order % 2 == 1, DEGREE - order, order) == 0
        for part in range(2):
            row = (p * 2 + part) * 128
            squares = jnp.zeros((128, 128), F32)
            for jb in range(8):
                values = spec[row : row + 128, jb * 128 : (jb + 1) * 128].astype(F32)
                squares = squares + values * values
            weight = jnp.where(is_even, jnp.where(has_zero, 1.0 - part, 2.0), 2.0)
            energy = energy + weight * jnp.sum(squares.T, axis=0, keepdims=True)
    e_mine[0] = energy
    e_plane[place] = energy

    def tell(t, carry):
        target = at(0, t // 8, (t // 2) % 4, t % 2)
        pltpu.make_async_remote_copy(
            src_ref=e_mine.at[0], dst_ref=e_plane.at[place], send_sem=e_sems.at[0], recv_sem=e_sems.at[1],
            device_id={"blk": target}, device_id_type=MESH,
        ).start()
        return carry

    lax.fori_loop(1, PLANE, tell, 0)

    def basis_step(step, carry):
        a, part = step // 16, step % 16
        back, sub = part // 4, part % 4
        first = (z + 4 - back) % 4 * 64 + sub * 16
        col = pl.multiple_of(a * 128, 128)
        for p in range(2):
            order = order_cols[pl.ds(first + p, 8, stride=2), :]
            even = jnp.where((order & 1) == 1, DEGREE - order, order)
            k = lax.broadcasted_iota(I32, (8, 128), 1) + a * 128
            for parity in range(2):
                m = even if parity == 0 else DEGREE - even
                cosine, sine = sincos(m * k)
                factor = jnp.where(m == 0, 1.0, 2.0)
                row = pl.multiple_of(parity * COLS + back * 128 + p * 64 + sub * 8, 8)
                basis[pl.ds(row, 8), pl.ds(col, 128)] = (factor * cosine).astype(BF16)
                row = pl.multiple_of(parity * COLS + back * 128 + p * 64 + 32 + sub * 8, 8)
                basis[pl.ds(row, 8), pl.ds(col, 128)] = (-factor * sine).astype(BF16)
        return carry

    lax.fori_loop(0, 256, basis_step, 0)

    told = pltpu.make_async_remote_copy(
        src_ref=e_plane.at[pl.ds(0, PLANE - 1)], dst_ref=e_plane.at[pl.ds(0, PLANE - 1)],
        send_sem=e_sems.at[0], recv_sem=e_sems.at[1], device_id={"blk": at(0, 0, 0, 1)}, device_id_type=MESH,
    )
    told.wait_send()
    told.wait_recv()
    total = e_plane[0]
    for s in range(1, PLANE):
        total = total + e_plane[s]
    e_mine[1] = total
    e_all[z] = total
    for d in range(1, 4):
        pltpu.make_async_remote_copy(
            src_ref=e_mine.at[1], dst_ref=e_all.at[z], send_sem=e_sems.at[2], recv_sem=e_sems.at[3],
            device_id={"blk": at(d, 0, 0, 0)}, device_id_type=MESH,
        ).start()

    for back in (0, 2, 1, 3):
        plane = (z + 4 - back) % 4
        count = PLANE - 1 if back == 0 else PLANE
        come = pltpu.make_async_remote_copy(
            src_ref=outbox.at[pl.ds(0, count)], dst_ref=inbox.at[pl.ds(0, count)],
            send_sem=send_sem, recv_sem=recv_sem.at[back], device_id={"blk": at(0, 0, 0, 1)}, device_id_type=MESH,
        )
        come.wait_recv()
        for g in range(4):
            wide[g] = (
                inbox[pl.ds(plane * PLANE, PLANE), :, g * 128 : (g + 1) * 128].astype(F32).reshape(256, 128)
            )
        for i in range(8):
            block = jnp.concatenate([wide[g, pl.ds(i, PLANE, stride=8), :] for g in range(4)], axis=0)
            block = block.T.astype(BF16)
            even_x[i * 64 : (i + 1) * 64, back * 128 : (back + 1) * 128] = block[:64]
            odd_x[i * 64 : (i + 1) * 64, back * 128 : (back + 1) * 128] = block[64:]

    told = pltpu.make_async_remote_copy(
        src_ref=e_all.at[pl.ds(0, 3)], dst_ref=e_all.at[pl.ds(0, 3)],
        send_sem=e_sems.at[2], recv_sem=e_sems.at[3], device_id={"blk": at(0, 0, 0, 1)}, device_id_type=MESH,
    )
    told.wait_send()
    told.wait_recv()
    energy_ref[...] = (e_all[0] + e_all[1]) + (e_all[2] + e_all[3])
    sent = pltpu.make_async_remote_copy(
        src_ref=outbox.at[pl.ds(0, NBLK - 1)], dst_ref=inbox.at[pl.ds(0, NBLK - 1)],
        send_sem=send_sem, recv_sem=recv_sem.at[0], device_id={"blk": at(0, 0, 0, 1)}, device_id_type=MESH,
    )
    sent.wait_send()


def synthesize(energy_in, even_x, odd_x, basis, potential_hbm, energy_ref, tile, tile_sems):
    both = energy_in[...]
    energy_ref[...] = (both[:, :FIELDS] + both[:, FIELDS:]) * (1.0 / NLAT)
    steps = HALF // 256

    def out_copy(step, half):
        return pltpu.make_async_copy(
            tile.at[step, half],
            potential_hbm.at[:, :, pl.ds(half * HALF + step * 256, 256)],
            tile_sems.at[step, half],
        )

    for n in range(steps):
        evens = jnp.dot(even_x[...], basis[:COLS, n * 256 : (n + 1) * 256], preferred_element_type=F32)
        odds = jnp.dot(odd_x[...], basis[COLS:, n * 256 : (n + 1) * 256], preferred_element_type=F32)
        tile[n, 0] = (evens + odds).astype(BF16).reshape(8, FIELDS, 256)
        tile[n, 1] = (evens - odds).astype(BF16).reshape(8, FIELDS, 256)
        for half in range(2):
            out_copy(n, half).start()
    for n in range(steps):
        for half in range(2):
            out_copy(n, half).wait()


def shards(load_coef, legendre, slab_orders, cycle_rows):
    any_space = pl.BlockSpec(memory_space=pl.ANY)
    vmem = pl.BlockSpec(memory_space=pltpu.VMEM)
    coef = load_coef.transpose(1, 0, 2)
    table = legendre.transpose(1, 0, 2).reshape(ROWS, 2, 8, 128).transpose(0, 2, 1, 3)
    even_x, odd_x, basis, energy = pl.pallas_call(
        exchange,
        out_shape=(
            jax.ShapeDtypeStruct((COLS, COLS), BF16),
            jax.ShapeDtypeStruct((COLS, COLS), BF16),
            jax.ShapeDtypeStruct((2 * COLS, HALF), BF16),
            jax.ShapeDtypeStruct((1, 128), F32),
        ),
        in_specs=[pl.BlockSpec(memory_space=pltpu.HBM)] * 4,
        out_specs=(vmem, vmem, vmem, vmem),
        scratch_shapes=[
            pltpu.VMEM((2, 128), I32),
            pltpu.VMEM((8, 128), I32),
            pltpu.VMEM((ROWS, 2, 128), BF16),
            pltpu.VMEM((8, ROWS, 2, 128), BF16),
            pltpu.VMEM((COLS, 2 * ROWS), BF16),
            pltpu.VMEM((COLS, NLAT), BF16),
            pltpu.VMEM((NLAT, NLAT), BF16),
            pltpu.VMEM((NBLK, 8, COLS), BF16),
            pltpu.VMEM((NBLK, 8, COLS), BF16),
            pltpu.VMEM((4, 256, 128), F32),
            pltpu.VMEM((256, 128), I32),
            pltpu.VMEM((2, 1, 128), F32),
            pltpu.VMEM((PLANE, 1, 128), F32),
            pltpu.VMEM((4, 1, 128), F32),
            pltpu.SemaphoreType.DMA((2,)),
            pltpu.SemaphoreType.DMA,
            pltpu.SemaphoreType.DMA((8,)),
            pltpu.SemaphoreType.DMA,
            pltpu.SemaphoreType.DMA((4,)),
            pltpu.SemaphoreType.DMA((4,)),
            pltpu.SemaphoreType.REGULAR((3,)),
        ],
        compiler_params=pltpu.CompilerParams(
            collective_id=0, has_side_effects=True, vmem_limit_bytes=44 * 1024 * 1024
        ),
        name="exchange",
    )(*[pltpu.with_memory_space_constraint(a, pltpu.HBM) for a in (slab_orders.reshape(2, 128), cycle_rows.reshape(8, 128), coef, table)])
    potential, energy = pl.pallas_call(
        synthesize,
        out_shape=(
            jax.ShapeDtypeStruct((8, FIELDS, NLON), BF16),
            jax.ShapeDtypeStruct((1, FIELDS), F32),
        ),
        in_specs=[vmem, vmem, vmem, vmem],
        out_specs=(any_space, vmem),
        scratch_shapes=[
            pltpu.VMEM((8, 2, 8, FIELDS, 256), BF16),
            pltpu.SemaphoreType.DMA((8, 2)),
        ],
        compiler_params=pltpu.CompilerParams(vmem_limit_bytes=24 * 1024 * 1024),
        name="synthesize",
    )(energy, even_x, odd_x, basis)
    return potential, energy.reshape(FIELDS)


def solution(mesh):
    in_specs = (P("blk", None, "rep"), P("blk", None, None), P(), P())
    out_specs = (P("blk", "rep", None), P("rep"))
    return jax.shard_map(shards, mesh=mesh, in_specs=in_specs, out_specs=out_specs, check_vma=False)
```

```python
import math

import jax
import jax.numpy as jnp
from jax import lax
from jax.experimental import pallas as pl
from jax.experimental.pallas import tpu as pltpu
from jax.sharding import PartitionSpec as P

BF16 = jnp.bfloat16
F32 = jnp.float32
I32 = jnp.int32
MESH = pl.DeviceIdType.MESH
NLON = 4096
HALF = NLON // 2
DEGREE = 2047
ROWS = 2049
NLAT = 1024
FIELDS = 64
NBLK = 128
PLANE = 32
COLS = 512


def sincos(phase):
    turned = (phase + 512) & 4095
    quadrant = turned >> 10
    theta = ((turned & 1023) - 512).astype(F32) * (2.0 * math.pi / NLON)
    t2 = theta * theta
    s = theta * (1.0 + t2 * (-1.0 / 6 + t2 * (1.0 / 120 + t2 * (-1.0 / 5040 + t2 * (1.0 / 362880)))))
    c = 1.0 + t2 * (-0.5 + t2 * (1.0 / 24 + t2 * (-1.0 / 720 + t2 * (1.0 / 40320))))
    odd = (quadrant & 1) == 1
    cosine = jnp.where(odd, s, c)
    sine = jnp.where(odd, c, s)
    flip_cos = ((quadrant + 1) & 2) == 2
    flip_sin = (quadrant & 2) == 2
    return jnp.where(flip_cos, -cosine, cosine), jnp.where(flip_sin, -sine, sine)


def exchange(
    orders_hbm, cycles_hbm, coef_hbm, leg_hbm,
    even_x, odd_x, basis, energy_ref,
    orders_v, cycles, coef, leg, stacked, spec, onehot, outbox, inbox, wide, order_cols, e_mine, e_plane, e_all,
    small_sems, coef_sem, leg_sem, send_sem, recv_sem, e_sems, ring_sems,
):
    me = lax.axis_index("blk")
    z, y, x, c = me // 32, (me // 8) % 4, (me // 2) % 4, me % 2

    def at(dz, dy, dx, dc):
        return (((z + dz) % 4 * 4 + (y + dy) % 4) * 4 + (x + dx) % 4) * 2 + (c + dc) % 2

    near = [(d, 0, 0, 0) for d in (1, 2, 3)] + [(0, d, 0, 0) for d in (1, 2, 3)]
    near += [(0, 0, d, 0) for d in (1, 2, 3)] + [(0, 0, 0, 1)]

    orders_copy = pltpu.make_async_copy(orders_hbm, orders_v, small_sems.at[0])
    orders_copy.start()
    cycles_copy = pltpu.make_async_copy(cycles_hbm, cycles, small_sems.at[1])
    cycles_copy.start()
    coef_copy = pltpu.make_async_copy(coef_hbm, coef, coef_sem)
    coef_copy.start()
    leg_copies = [pltpu.make_async_copy(leg_hbm.at[:, jt], leg.at[jt], leg_sem.at[jt]) for jt in range(8)]

    barrier = pltpu.get_barrier_semaphore()

    def signal(sem):
        for offset in near:
            pl.semaphore_signal(sem, inc=1, device_id={"blk": at(*offset)}, device_id_type=MESH)

    signal(barrier)

    orders_copy.wait()
    for h in range(2):
        order_cols[h * 128 : (h + 1) * 128, :] = jnp.broadcast_to(orders_v[h : h + 1, :], (128, 128)).T
    cycles_copy.wait()
    lanes = lax.broadcasted_iota(I32, (128, 128), 1)

    def pick(ib, carry):
        wanted = jnp.broadcast_to(cycles[pl.ds(ib, 1), :], (128, 128)).T
        row = pl.multiple_of(ib * 128, 128)
        for jb in range(8):
            onehot[pl.ds(row, 128), jb * 128 : (jb + 1) * 128] = jnp.where(
                wanted == lanes + jb * 128, 1.0, 0.0
            ).astype(BF16)
        return carry

    lax.fori_loop(0, 8, pick, 0)

    coef_copy.wait()
    for copy in leg_copies[:4]:
        copy.start()
    packed = coef[...].reshape(2 * ROWS, 128).T
    column = lax.broadcasted_iota(I32, (1, 2 * ROWS), 1)
    row_id, pair_id = column >> 1, column & 1
    for p in range(2):
        order = order_cols[pl.ds(me * 2 + p, 1), :][:, :1]
        lower = jnp.where(row_id < DEGREE + 1 - order, 1, 0)
        parity_of = jnp.where(pair_id == p, (lower + order + 1) & 1, 2)
        for parity in range(2):
            keep = jnp.where(parity_of == parity, 1.0, 0.0).astype(BF16)
            for part in range(2):
                row = ((p * 2 + part) * 2 + parity) * 64
                stacked[row : row + 64, :] = packed[part * 64 : (part + 1) * 64] * keep

    pl.semaphore_wait(barrier, 10)
    signal(ring_sems.at[0])
    for copy in leg_copies[4:]:
        copy.start()

    def legs(jp, carry):
        for jt in range(2):
            pltpu.make_async_copy(leg_hbm.at[:, 2 * jp + jt], leg.at[2 * jp + jt], leg_sem.at[2 * jp + jt]).wait()
        table = jnp.concatenate(
            [leg[2 * jp].reshape(2 * ROWS, 128), leg[2 * jp + 1].reshape(2 * ROWS, 128)], axis=1
        )
        spec[:, pl.ds(pl.multiple_of(jp * 256, 256), 256)] = jnp.dot(
            stacked[...], table, preferred_element_type=F32
        ).astype(BF16)
        return carry

    lax.fori_loop(0, 3, legs, 0)
    pl.semaphore_wait(ring_sems.at[0], 10)
    signal(ring_sems.at[1])
    lax.fori_loop(3, 4, legs, 0)

    def choose(ib, carry):
        row = pl.multiple_of(ib * 256, 256)
        outbox[pl.ds(pl.multiple_of(ib * 32, 32), 32)] = (
            lax.dot_general(
                onehot[pl.ds(row, 256), :], spec[...], (((1,), (1,)), ((), ())), preferred_element_type=F32
            )
            .reshape(32, 8, COLS)
            .astype(BF16)
        )
        return carry

    lax.fori_loop(0, 4, choose, 0)

    def send(dz, dy, dx, dc):
        target = at(dz, dy, dx, dc)
        pltpu.make_async_remote_copy(
            src_ref=outbox.at[target], dst_ref=inbox.at[me], send_sem=send_sem, recv_sem=recv_sem.at[dz],
            device_id={"blk": target}, device_id_type=MESH,
        ).start()

    def send_all(planes, axes, flip):
        count = 3 ** len(axes)

        def one(t, carry):
            offset = [0, 0, 0, flip]
            rest = t
            for axis in axes:
                offset[axis] = rest % 3 + 1
                rest = rest // 3
            for dz in planes:
                send(dz, *offset[1:])
            return carry

        if count == 1:
            one(0, 0)
        else:
            lax.fori_loop(0, count, one, 0)

    across = (2, 1, 3)
    send_all(across, (), 0)
    send_all((2, 1, 3, 0), (2,), 0)
    send_all((2, 1, 3, 0), (1,), 0)
    send_all((2, 1, 3, 0), (), 1)
    for axes, flip in (((1, 2), 0), ((1,), 1), ((2,), 1)):
        send_all((0,), axes, flip)
    pl.semaphore_wait(ring_sems.at[1], 10)
    signal(ring_sems.at[2])
    for axes, flip in (((1, 2), 0), ((1,), 1), ((2,), 1)):
        send_all((2,), axes, flip)
    send_all((0,), (1, 2), 1)
    pl.semaphore_wait(ring_sems.at[2], 10)
    send_all((2,), (1, 2), 1)
    for axes, flip in (((1, 2), 0), ((1,), 1), ((2,), 1), ((1, 2), 1)):
        send_all((1, 3), axes, flip)
    inbox[me] = outbox[me]

    place = me % PLANE
    is_even = lax.broadcasted_iota(I32, (1, 128), 1) < FIELDS
    energy = jnp.zeros((1, 128), F32)
    for p in range(2):
        order = order_cols[pl.ds(me * 2 + p, 1), :]
        has_zero = jnp.where(order % 2 == 1, DEGREE - order, order) == 0
        for part in range(2):
            row = (p * 2 + part) * 128
            squares = jnp.zeros((128, 128), F32)
            for jb in range(8):
                values = spec[row : row + 128, jb * 128 : (jb + 1) * 128].astype(F32)
                squares = squares + values * values
            weight = jnp.where(is_even, jnp.where(has_zero, 1.0 - part, 2.0), 2.0)
            energy = energy + weight * jnp.sum(squares.T, axis=0, keepdims=True)
    e_mine[0] = energy
    e_plane[place] = energy

    def tell(t, carry):
        target = at(0, t // 8, (t // 2) % 4, t % 2)
        pltpu.make_async_remote_copy(
            src_ref=e_mine.at[0], dst_ref=e_plane.at[place], send_sem=e_sems.at[0], recv_sem=e_sems.at[1],
            device_id={"blk": target}, device_id_type=MESH,
        ).start()
        return carry

    lax.fori_loop(1, PLANE, tell, 0)

    def basis_step(step, carry):
        a, part = step // 16, step % 16
        back, sub = part // 4, part % 4
        first = (z + 4 - back) % 4 * 64 + sub * 16
        col = pl.multiple_of(a * 128, 128)
        for p in range(2):
            order = order_cols[pl.ds(first + p, 8, stride=2), :]
            even = jnp.where((order & 1) == 1, DEGREE - order, order)
            k = lax.broadcasted_iota(I32, (8, 128), 1) + a * 128
            for parity in range(2):
                m = even if parity == 0 else DEGREE - even
                cosine, sine = sincos(m * k)
                factor = jnp.where(m == 0, 1.0, 2.0)
                row = pl.multiple_of(parity * COLS + back * 128 + p * 64 + sub * 8, 8)
                basis[pl.ds(row, 8), pl.ds(col, 128)] = (factor * cosine).astype(BF16)
                row = pl.multiple_of(parity * COLS + back * 128 + p * 64 + 32 + sub * 8, 8)
                basis[pl.ds(row, 8), pl.ds(col, 128)] = (-factor * sine).astype(BF16)
        return carry

    lax.fori_loop(0, 256, basis_step, 0)

    told = pltpu.make_async_remote_copy(
        src_ref=e_plane.at[pl.ds(0, PLANE - 1)], dst_ref=e_plane.at[pl.ds(0, PLANE - 1)],
        send_sem=e_sems.at[0], recv_sem=e_sems.at[1], device_id={"blk": at(0, 0, 0, 1)}, device_id_type=MESH,
    )
    told.wait_send()
    told.wait_recv()
    total = e_plane[0]
    for s in range(1, PLANE):
        total = total + e_plane[s]
    e_mine[1] = total
    e_all[z] = total
    for d in range(1, 4):
        pltpu.make_async_remote_copy(
            src_ref=e_mine.at[1], dst_ref=e_all.at[z], send_sem=e_sems.at[2], recv_sem=e_sems.at[3],
            device_id={"blk": at(d, 0, 0, 0)}, device_id_type=MESH,
        ).start()

    def landed(back, count):
        pltpu.make_async_remote_copy(
            src_ref=outbox.at[pl.ds(0, count)], dst_ref=inbox.at[pl.ds(0, count)],
            send_sem=send_sem, recv_sem=recv_sem.at[back], device_id={"blk": at(0, 0, 0, 1)}, device_id_type=MESH,
        ).wait_recv()

    def build(step, carry):
        back = (2 * step) % 3 + step // 3 * 3
        plane = (z + 4 - back) % 4
        @pl.when(step == 0)
        def _():
            landed(0, PLANE - 1)

        @pl.when(step > 0)
        def _():
            landed(back, PLANE)

        for g in range(4):
            wide[g] = inbox[pl.ds(plane * PLANE, PLANE), :, g * 128 : (g + 1) * 128].astype(F32).reshape(256, 128)
        col = pl.multiple_of(back * 128, 128)
        for i in range(8):
            block = jnp.concatenate([wide[g, pl.ds(i, PLANE, stride=8), :] for g in range(4)], axis=0)
            block = block.T.astype(BF16)
            even_x[i * 64 : (i + 1) * 64, pl.ds(col, 128)] = block[:64]
            odd_x[i * 64 : (i + 1) * 64, pl.ds(col, 128)] = block[64:]
        return carry

    lax.fori_loop(0, 4, build, 0)

    told = pltpu.make_async_remote_copy(
        src_ref=e_all.at[pl.ds(0, 3)], dst_ref=e_all.at[pl.ds(0, 3)],
        send_sem=e_sems.at[2], recv_sem=e_sems.at[3], device_id={"blk": at(0, 0, 0, 1)}, device_id_type=MESH,
    )
    told.wait_send()
    told.wait_recv()
    energy_ref[...] = (e_all[0] + e_all[1]) + (e_all[2] + e_all[3])
    sent = pltpu.make_async_remote_copy(
        src_ref=outbox.at[pl.ds(0, NBLK - 1)], dst_ref=inbox.at[pl.ds(0, NBLK - 1)],
        send_sem=send_sem, recv_sem=recv_sem.at[0], device_id={"blk": at(0, 0, 0, 1)}, device_id_type=MESH,
    )
    sent.wait_send()


def synthesize(energy_in, even_x, odd_x, basis, potential_hbm, energy_ref, tile, tile_sems):
    both = energy_in[...]
    energy_ref[...] = (both[:, :FIELDS] + both[:, FIELDS:]) * (1.0 / NLAT)
    steps = HALF // 256

    def out_copy(step, half):
        first = pl.multiple_of(half * HALF + step * 256, 256)
        return pltpu.make_async_copy(
            tile.at[step, half], potential_hbm.at[:, :, pl.ds(first, 256)], tile_sems.at[step, half]
        )

    def columns(n, carry):
        at = pl.ds(pl.multiple_of(n * 256, 256), 256)
        evens = jnp.dot(even_x[...], basis[:COLS, at], preferred_element_type=F32)
        odds = jnp.dot(odd_x[...], basis[COLS:, at], preferred_element_type=F32)
        tile[n, 0] = (evens + odds).astype(BF16).reshape(8, FIELDS, 256)
        tile[n, 1] = (evens - odds).astype(BF16).reshape(8, FIELDS, 256)
        for half in range(2):
            out_copy(n, half).start()
        return carry

    def finish(n, carry):
        for half in range(2):
            out_copy(n, half).wait()
        return carry

    lax.fori_loop(0, steps, columns, 0)
    lax.fori_loop(0, steps, finish, 0)


def shards(load_coef, legendre, slab_orders, cycle_rows):
    any_space = pl.BlockSpec(memory_space=pl.ANY)
    vmem = pl.BlockSpec(memory_space=pltpu.VMEM)
    coef = load_coef.transpose(1, 0, 2)
    table = legendre.transpose(1, 0, 2).reshape(ROWS, 2, 8, 128).transpose(0, 2, 1, 3)
    even_x, odd_x, basis, energy = pl.pallas_call(
        exchange,
        out_shape=(
            jax.ShapeDtypeStruct((COLS, COLS), BF16),
            jax.ShapeDtypeStruct((COLS, COLS), BF16),
            jax.ShapeDtypeStruct((2 * COLS, HALF), BF16),
            jax.ShapeDtypeStruct((1, 128), F32),
        ),
        in_specs=[pl.BlockSpec(memory_space=pltpu.HBM)] * 4,
        out_specs=(vmem, vmem, vmem, vmem),
        scratch_shapes=[
            pltpu.VMEM((2, 128), I32),
            pltpu.VMEM((8, 128), I32),
            pltpu.VMEM((ROWS, 2, 128), BF16),
            pltpu.VMEM((8, ROWS, 2, 128), BF16),
            pltpu.VMEM((COLS, 2 * ROWS), BF16),
            pltpu.VMEM((COLS, NLAT), BF16),
            pltpu.VMEM((NLAT, NLAT), BF16),
            pltpu.VMEM((NBLK, 8, COLS), BF16),
            pltpu.VMEM((NBLK, 8, COLS), BF16),
            pltpu.VMEM((4, 256, 128), F32),
            pltpu.VMEM((256, 128), I32),
            pltpu.VMEM((2, 1, 128), F32),
            pltpu.VMEM((PLANE, 1, 128), F32),
            pltpu.VMEM((4, 1, 128), F32),
            pltpu.SemaphoreType.DMA((2,)),
            pltpu.SemaphoreType.DMA,
            pltpu.SemaphoreType.DMA((8,)),
            pltpu.SemaphoreType.DMA,
            pltpu.SemaphoreType.DMA((4,)),
            pltpu.SemaphoreType.DMA((4,)),
            pltpu.SemaphoreType.REGULAR((3,)),
        ],
        compiler_params=pltpu.CompilerParams(
            collective_id=0, has_side_effects=True, vmem_limit_bytes=44 * 1024 * 1024
        ),
        name="exchange",
    )(*[pltpu.with_memory_space_constraint(a, pltpu.HBM) for a in (slab_orders.reshape(2, 128), cycle_rows.reshape(8, 128), coef, table)])
    potential, energy = pl.pallas_call(
        synthesize,
        out_shape=(
            jax.ShapeDtypeStruct((8, FIELDS, NLON), BF16),
            jax.ShapeDtypeStruct((1, FIELDS), F32),
        ),
        in_specs=[vmem, vmem, vmem, vmem],
        out_specs=(any_space, vmem),
        scratch_shapes=[
            pltpu.VMEM((8, 2, 8, FIELDS, 256), BF16),
            pltpu.SemaphoreType.DMA((8, 2)),
        ],
        compiler_params=pltpu.CompilerParams(vmem_limit_bytes=24 * 1024 * 1024),
        name="synthesize",
    )(energy, even_x, odd_x, basis)
    return potential, energy.reshape(FIELDS)


def solution(mesh):
    in_specs = (P("blk", None, "rep"), P("blk", None, None), P(), P())
    out_specs = (P("blk", "rep", None), P("rep"))
    return jax.shard_map(shards, mesh=mesh, in_specs=in_specs, out_specs=out_specs, check_vma=False)
```

```python
import math

import jax
import jax.numpy as jnp
from jax import lax
from jax.experimental import pallas as pl
from jax.experimental.pallas import tpu as pltpu
from jax.sharding import PartitionSpec as P

BF16 = jnp.bfloat16
F32 = jnp.float32
I32 = jnp.int32
MESH = pl.DeviceIdType.MESH
NLON = 4096
HALF = NLON // 2
DEGREE = 2047
ROWS = 2049
NLAT = 1024
FIELDS = 64
NBLK = 128
PLANE = 32
COLS = 512


def sincos(phase):
    turned = (phase + 512) & 4095
    quadrant = turned >> 10
    theta = ((turned & 1023) - 512).astype(F32) * (2.0 * math.pi / NLON)
    t2 = theta * theta
    s = theta * (1.0 + t2 * (-1.0 / 6 + t2 * (1.0 / 120 + t2 * (-1.0 / 5040 + t2 * (1.0 / 362880)))))
    c = 1.0 + t2 * (-0.5 + t2 * (1.0 / 24 + t2 * (-1.0 / 720 + t2 * (1.0 / 40320))))
    odd = (quadrant & 1) == 1
    cosine = jnp.where(odd, s, c)
    sine = jnp.where(odd, c, s)
    flip_cos = ((quadrant + 1) & 2) == 2
    flip_sin = (quadrant & 2) == 2
    return jnp.where(flip_cos, -cosine, cosine), jnp.where(flip_sin, -sine, sine)


def exchange(
    orders_hbm, cycles_hbm, coef_hbm, leg_hbm,
    even_x, odd_x, basis, evens, odds, energy_ref,
    orders_v, cycles, coef, leg, first_x, stacked, spec, onehot, outbox, inbox, wide, order_cols, e_mine, e_plane, e_all,
    small_sems, coef_sem, leg_sem, send_sem, recv_sem, e_sems, ring_sems,
):
    me = lax.axis_index("blk")
    z, y, x, c = me // 32, (me // 8) % 4, (me // 2) % 4, me % 2

    def at(dz, dy, dx, dc):
        return (((z + dz) % 4 * 4 + (y + dy) % 4) * 4 + (x + dx) % 4) * 2 + (c + dc) % 2

    near = [(d, 0, 0, 0) for d in (1, 2, 3)] + [(0, d, 0, 0) for d in (1, 2, 3)]
    near += [(0, 0, d, 0) for d in (1, 2, 3)] + [(0, 0, 0, 1)]

    orders_copy = pltpu.make_async_copy(orders_hbm, orders_v, small_sems.at[0])
    orders_copy.start()
    cycles_copy = pltpu.make_async_copy(cycles_hbm, cycles, small_sems.at[1])
    cycles_copy.start()
    coef_copy = pltpu.make_async_copy(coef_hbm, coef, coef_sem)
    coef_copy.start()
    leg_copies = [pltpu.make_async_copy(leg_hbm.at[:, jt], leg.at[jt], leg_sem.at[jt]) for jt in range(8)]

    barrier = pltpu.get_barrier_semaphore()

    def signal(sem):
        for offset in near:
            pl.semaphore_signal(sem, inc=1, device_id={"blk": at(*offset)}, device_id_type=MESH)

    signal(barrier)

    orders_copy.wait()
    for h in range(2):
        order_cols[h * 128 : (h + 1) * 128, :] = jnp.broadcast_to(orders_v[h : h + 1, :], (128, 128)).T
    cycles_copy.wait()
    lanes = lax.broadcasted_iota(I32, (128, 128), 1)

    def pick(ib, carry):
        wanted = jnp.broadcast_to(cycles[pl.ds(ib, 1), :], (128, 128)).T
        row = pl.multiple_of(ib * 128, 128)
        for jb in range(8):
            onehot[pl.ds(row, 128), jb * 128 : (jb + 1) * 128] = jnp.where(
                wanted == lanes + jb * 128, 1.0, 0.0
            ).astype(BF16)
        return carry

    lax.fori_loop(0, 8, pick, 0)

    coef_copy.wait()
    for copy in leg_copies[:4]:
        copy.start()
    packed = coef[...].reshape(2 * ROWS, 128).T
    column = lax.broadcasted_iota(I32, (1, 2 * ROWS), 1)
    row_id, pair_id = column >> 1, column & 1
    for p in range(2):
        order = order_cols[pl.ds(me * 2 + p, 1), :][:, :1]
        lower = jnp.where(row_id < DEGREE + 1 - order, 1, 0)
        parity_of = jnp.where(pair_id == p, (lower + order + 1) & 1, 2)
        for parity in range(2):
            keep = jnp.where(parity_of == parity, 1.0, 0.0).astype(BF16)
            for part in range(2):
                row = ((p * 2 + part) * 2 + parity) * 64
                stacked[row : row + 64, :] = packed[part * 64 : (part + 1) * 64] * keep

    pl.semaphore_wait(barrier, 10)
    signal(ring_sems.at[0])
    for copy in leg_copies[4:]:
        copy.start()

    def legs(jp, carry):
        for jt in range(2):
            pltpu.make_async_copy(leg_hbm.at[:, 2 * jp + jt], leg.at[2 * jp + jt], leg_sem.at[2 * jp + jt]).wait()
        table = jnp.concatenate(
            [leg[2 * jp].reshape(2 * ROWS, 128), leg[2 * jp + 1].reshape(2 * ROWS, 128)], axis=1
        )
        spec[:, pl.ds(pl.multiple_of(jp * 256, 256), 256)] = jnp.dot(
            stacked[...], table, preferred_element_type=F32
        ).astype(BF16)
        return carry

    lax.fori_loop(0, 3, legs, 0)
    pl.semaphore_wait(ring_sems.at[0], 10)
    signal(ring_sems.at[1])
    lax.fori_loop(3, 4, legs, 0)

    def choose(ib, carry):
        row = pl.multiple_of(ib * 256, 256)
        outbox[pl.ds(pl.multiple_of(ib * 32, 32), 32)] = (
            lax.dot_general(
                onehot[pl.ds(row, 256), :], spec[...], (((1,), (1,)), ((), ())), preferred_element_type=F32
            )
            .reshape(32, 8, COLS)
            .astype(BF16)
        )
        return carry

    lax.fori_loop(0, 4, choose, 0)

    def send(dz, dy, dx, dc):
        target = at(dz, dy, dx, dc)
        pltpu.make_async_remote_copy(
            src_ref=outbox.at[target], dst_ref=inbox.at[me], send_sem=send_sem, recv_sem=recv_sem.at[dz],
            device_id={"blk": target}, device_id_type=MESH,
        ).start()

    def send_all(planes, axes, flip):
        count = 3 ** len(axes)

        def one(t, carry):
            offset = [0, 0, 0, flip]
            rest = t
            for axis in axes:
                offset[axis] = rest % 3 + 1
                rest = rest // 3
            for dz in planes:
                send(dz, *offset[1:])
            return carry

        if count == 1:
            one(0, 0)
        else:
            lax.fori_loop(0, count, one, 0)

    across = (2, 1, 3)
    send_all(across, (), 0)
    send_all((2, 1, 3, 0), (2,), 0)
    send_all((2, 1, 3, 0), (1,), 0)
    send_all((2, 1, 3, 0), (), 1)
    for axes, flip in (((1, 2), 0), ((1,), 1), ((2,), 1)):
        send_all((0,), axes, flip)
    pl.semaphore_wait(ring_sems.at[1], 10)
    signal(ring_sems.at[2])
    for axes, flip in (((1, 2), 0), ((1,), 1), ((2,), 1)):
        send_all((2,), axes, flip)
    send_all((0,), (1, 2), 1)
    pl.semaphore_wait(ring_sems.at[2], 10)
    send_all((2,), (1, 2), 1)
    for axes, flip in (((1, 2), 0), ((1,), 1), ((2,), 1), ((1, 2), 1)):
        send_all((1, 3), axes, flip)
    inbox[me] = outbox[me]

    place = me % PLANE
    is_even = lax.broadcasted_iota(I32, (1, 128), 1) < FIELDS
    energy = jnp.zeros((1, 128), F32)
    for p in range(2):
        order = order_cols[pl.ds(me * 2 + p, 1), :]
        has_zero = jnp.where(order % 2 == 1, DEGREE - order, order) == 0
        for part in range(2):
            row = (p * 2 + part) * 128
            squares = jnp.zeros((128, 128), F32)
            for jb in range(8):
                values = spec[row : row + 128, jb * 128 : (jb + 1) * 128].astype(F32)
                squares = squares + values * values
            weight = jnp.where(is_even, jnp.where(has_zero, 1.0 - part, 2.0), 2.0)
            energy = energy + weight * jnp.sum(squares.T, axis=0, keepdims=True)
    e_mine[0] = energy
    e_plane[place] = energy

    def tell(t, carry):
        target = at(0, t // 8, (t // 2) % 4, t % 2)
        pltpu.make_async_remote_copy(
            src_ref=e_mine.at[0], dst_ref=e_plane.at[place], send_sem=e_sems.at[0], recv_sem=e_sems.at[1],
            device_id={"blk": target}, device_id_type=MESH,
        ).start()
        return carry

    lax.fori_loop(1, PLANE, tell, 0)

    def back_of(slot):
        return (2 * slot) % 3 + slot // 3 * 3

    def basis_step(step, carry):
        a, part = step // 16, step % 16
        slot, sub = part // 4, part % 4
        first = (z + 4 - back_of(slot)) % 4 * 64 + sub * 16
        col = pl.multiple_of(a * 128, 128)
        for p in range(2):
            order = order_cols[pl.ds(first + p, 8, stride=2), :]
            even = jnp.where((order & 1) == 1, DEGREE - order, order)
            k = lax.broadcasted_iota(I32, (8, 128), 1) + a * 128
            for parity in range(2):
                m = even if parity == 0 else DEGREE - even
                cosine, sine = sincos(m * k)
                factor = jnp.where(m == 0, 1.0, 2.0)
                row = pl.multiple_of(parity * COLS + slot * 128 + p * 64 + sub * 8, 8)
                basis[pl.ds(row, 8), pl.ds(col, 128)] = (factor * cosine).astype(BF16)
                row = pl.multiple_of(parity * COLS + slot * 128 + p * 64 + 32 + sub * 8, 8)
                basis[pl.ds(row, 8), pl.ds(col, 128)] = (-factor * sine).astype(BF16)
        return carry

    lax.fori_loop(0, 256, basis_step, 0)

    told = pltpu.make_async_remote_copy(
        src_ref=e_plane.at[pl.ds(0, PLANE - 1)], dst_ref=e_plane.at[pl.ds(0, PLANE - 1)],
        send_sem=e_sems.at[0], recv_sem=e_sems.at[1], device_id={"blk": at(0, 0, 0, 1)}, device_id_type=MESH,
    )
    told.wait_send()
    told.wait_recv()
    total = e_plane[0]
    for s in range(1, PLANE):
        total = total + e_plane[s]
    e_mine[1] = total
    e_all[z] = total
    for d in range(1, 4):
        pltpu.make_async_remote_copy(
            src_ref=e_mine.at[1], dst_ref=e_all.at[z], send_sem=e_sems.at[2], recv_sem=e_sems.at[3],
            device_id={"blk": at(d, 0, 0, 0)}, device_id_type=MESH,
        ).start()

    def landed(back, count):
        pltpu.make_async_remote_copy(
            src_ref=outbox.at[pl.ds(0, count)], dst_ref=inbox.at[pl.ds(0, count)],
            send_sem=send_sem, recv_sem=recv_sem.at[back], device_id={"blk": at(0, 0, 0, 1)}, device_id_type=MESH,
        ).wait_recv()

    def build(slot, even_to, odd_to):
        back = back_of(slot)
        plane = (z + 4 - back) % 4
        @pl.when(slot == 0)
        def _():
            landed(0, PLANE - 1)

        @pl.when(slot > 0)
        def _():
            landed(back, PLANE)

        for g in range(4):
            wide[g] = inbox[pl.ds(plane * PLANE, PLANE), :, g * 128 : (g + 1) * 128].astype(F32).reshape(256, 128)
        col = pl.multiple_of(slot % 2 * 128, 128)
        for i in range(8):
            block = jnp.concatenate([wide[g, pl.ds(i, PLANE, stride=8), :] for g in range(4)], axis=0)
            block = block.T.astype(BF16)
            even_to[i * 64 : (i + 1) * 64, pl.ds(col, 128)] = block[:64]
            odd_to[i * 64 : (i + 1) * 64, pl.ds(col, 128)] = block[64:]

    def build_first(slot, carry):
        build(slot, first_x.at[0], first_x.at[1])
        return carry

    def build_last(slot, carry):
        build(slot, even_x, odd_x)
        return carry

    def sum_first(n, carry):
        cols = pl.ds(pl.multiple_of(n * 256, 256), 256)
        evens[:, cols] = jnp.dot(first_x[0], basis[:256, cols], preferred_element_type=F32)
        odds[:, cols] = jnp.dot(first_x[1], basis[COLS : COLS + 256, cols], preferred_element_type=F32)
        return carry

    lax.fori_loop(0, 2, build_first, 0)
    lax.fori_loop(0, 8, sum_first, 0)
    lax.fori_loop(2, 4, build_last, 0)

    told = pltpu.make_async_remote_copy(
        src_ref=e_all.at[pl.ds(0, 3)], dst_ref=e_all.at[pl.ds(0, 3)],
        send_sem=e_sems.at[2], recv_sem=e_sems.at[3], device_id={"blk": at(0, 0, 0, 1)}, device_id_type=MESH,
    )
    told.wait_send()
    told.wait_recv()
    energy_ref[...] = (e_all[0] + e_all[1]) + (e_all[2] + e_all[3])
    sent = pltpu.make_async_remote_copy(
        src_ref=outbox.at[pl.ds(0, NBLK - 1)], dst_ref=inbox.at[pl.ds(0, NBLK - 1)],
        send_sem=send_sem, recv_sem=recv_sem.at[0], device_id={"blk": at(0, 0, 0, 1)}, device_id_type=MESH,
    )
    sent.wait_send()


def synthesize(energy_in, even_x, odd_x, basis, evens, odds, potential_hbm, energy_ref, tile, tile_sems):
    both = energy_in[...]
    energy_ref[...] = (both[:, :FIELDS] + both[:, FIELDS:]) * (1.0 / NLAT)
    steps = HALF // 256
    copies = []
    for n in range(steps):
        cols = slice(n * 256, (n + 1) * 256)
        even = evens[:, cols] + jnp.dot(even_x[...], basis[256:COLS, cols], preferred_element_type=F32)
        odd = odds[:, cols] + jnp.dot(odd_x[...], basis[COLS + 256 :, cols], preferred_element_type=F32)
        for half in range(2):
            tile[n, half] = (even + odd if half == 0 else even - odd).astype(BF16).reshape(8, FIELDS, 256)
            copy = pltpu.make_async_copy(
                tile.at[n, half], potential_hbm.at[:, :, pl.ds(half * HALF + n * 256, 256)], tile_sems.at[n, half]
            )
            copy.start()
            copies.append(copy)
    for copy in copies:
        copy.wait()


def shards(load_coef, legendre, slab_orders, cycle_rows):
    any_space = pl.BlockSpec(memory_space=pl.ANY)
    vmem = pl.BlockSpec(memory_space=pltpu.VMEM)
    coef = load_coef.transpose(1, 0, 2)
    table = legendre.transpose(1, 0, 2).reshape(ROWS, 2, 8, 128).transpose(0, 2, 1, 3)
    even_x, odd_x, basis, evens, odds, energy = pl.pallas_call(
        exchange,
        out_shape=(
            jax.ShapeDtypeStruct((COLS, 256), BF16),
            jax.ShapeDtypeStruct((COLS, 256), BF16),
            jax.ShapeDtypeStruct((2 * COLS, HALF), BF16),
            jax.ShapeDtypeStruct((COLS, HALF), F32),
            jax.ShapeDtypeStruct((COLS, HALF), F32),
            jax.ShapeDtypeStruct((1, 128), F32),
        ),
        in_specs=[pl.BlockSpec(memory_space=pltpu.HBM)] * 4,
        out_specs=(vmem,) * 6,
        scratch_shapes=[
            pltpu.VMEM((2, 128), I32),
            pltpu.VMEM((8, 128), I32),
            pltpu.VMEM((ROWS, 2, 128), BF16),
            pltpu.VMEM((8, ROWS, 2, 128), BF16),
            pltpu.VMEM((2, COLS, 256), BF16),
            pltpu.VMEM((COLS, 2 * ROWS), BF16),
            pltpu.VMEM((COLS, NLAT), BF16),
            pltpu.VMEM((NLAT, NLAT), BF16),
            pltpu.VMEM((NBLK, 8, COLS), BF16),
            pltpu.VMEM((NBLK, 8, COLS), BF16),
            pltpu.VMEM((4, 256, 128), F32),
            pltpu.VMEM((256, 128), I32),
            pltpu.VMEM((2, 1, 128), F32),
            pltpu.VMEM((PLANE, 1, 128), F32),
            pltpu.VMEM((4, 1, 128), F32),
            pltpu.SemaphoreType.DMA((2,)),
            pltpu.SemaphoreType.DMA,
            pltpu.SemaphoreType.DMA((8,)),
            pltpu.SemaphoreType.DMA,
            pltpu.SemaphoreType.DMA((4,)),
            pltpu.SemaphoreType.DMA((4,)),
            pltpu.SemaphoreType.REGULAR((3,)),
        ],
        compiler_params=pltpu.CompilerParams(
            collective_id=0, has_side_effects=True, vmem_limit_bytes=36 * 1024 * 1024
        ),
        name="exchange",
    )(*[pltpu.with_memory_space_constraint(a, pltpu.HBM) for a in (slab_orders.reshape(2, 128), cycle_rows.reshape(8, 128), coef, table)])
    potential, energy = pl.pallas_call(
        synthesize,
        out_shape=(
            jax.ShapeDtypeStruct((8, FIELDS, NLON), BF16),
            jax.ShapeDtypeStruct((1, FIELDS), F32),
        ),
        in_specs=[vmem] * 6,
        out_specs=(any_space, vmem),
        scratch_shapes=[
            pltpu.VMEM((8, 2, 8, FIELDS, 256), BF16),
            pltpu.SemaphoreType.DMA((8, 2)),
        ],
        compiler_params=pltpu.CompilerParams(vmem_limit_bytes=20 * 1024 * 1024),
        name="synthesize",
    )(energy, even_x, odd_x, basis, evens, odds)
    return potential, energy.reshape(FIELDS)


def solution(mesh):
    in_specs = (P("blk", None, "rep"), P("blk", None, None), P(), P())
    out_specs = (P("blk", "rep", None), P("rep"))
    return jax.shard_map(shards, mesh=mesh, in_specs=in_specs, out_specs=out_specs, check_vma=False)
```

```python
import math

import jax
import jax.numpy as jnp
from jax import lax
from jax.experimental import pallas as pl
from jax.experimental.pallas import tpu as pltpu
from jax.sharding import PartitionSpec as P

BF16 = jnp.bfloat16
F32 = jnp.float32
I32 = jnp.int32
MESH = pl.DeviceIdType.MESH
NLON = 4096
HALF = NLON // 2
DEGREE = 2047
ROWS = 2049
NLAT = 1024
FIELDS = 64
NBLK = 128
PLANE = 32
COLS = 512


def sincos(phase):
    turned = (phase + 512) & 4095
    quadrant = turned >> 10
    theta = ((turned & 1023) - 512).astype(F32) * (2.0 * math.pi / NLON)
    t2 = theta * theta
    s = theta * (1.0 + t2 * (-1.0 / 6 + t2 * (1.0 / 120 + t2 * (-1.0 / 5040 + t2 * (1.0 / 362880)))))
    c = 1.0 + t2 * (-0.5 + t2 * (1.0 / 24 + t2 * (-1.0 / 720 + t2 * (1.0 / 40320))))
    odd = (quadrant & 1) == 1
    cosine = jnp.where(odd, s, c)
    sine = jnp.where(odd, c, s)
    flip_cos = ((quadrant + 1) & 2) == 2
    flip_sin = (quadrant & 2) == 2
    return jnp.where(flip_cos, -cosine, cosine), jnp.where(flip_sin, -sine, sine)


def exchange(
    orders_hbm, cycles_hbm, coef_hbm, leg_hbm,
    even_x, odd_x, basis, evens, odds, energy_ref,
    orders_v, cycles, coef, leg, first_x, stacked, spec, onehot, outbox, inbox, wide, order_cols, e_mine, e_plane, e_all,
    small_sems, coef_sem, leg_sem, send_sem, recv_sem, e_sems, ring_sems,
):
    me = lax.axis_index("blk")
    z, y, x, c = me // 32, (me // 8) % 4, (me // 2) % 4, me % 2

    def at(dz, dy, dx, dc):
        return (((z + dz) % 4 * 4 + (y + dy) % 4) * 4 + (x + dx) % 4) * 2 + (c + dc) % 2

    near = [(d, 0, 0, 0) for d in (1, 2, 3)] + [(0, d, 0, 0) for d in (1, 2, 3)]
    near += [(0, 0, d, 0) for d in (1, 2, 3)] + [(0, 0, 0, 1)]

    orders_copy = pltpu.make_async_copy(orders_hbm, orders_v, small_sems.at[0])
    orders_copy.start()
    cycles_copy = pltpu.make_async_copy(cycles_hbm, cycles, small_sems.at[1])
    cycles_copy.start()
    coef_copy = pltpu.make_async_copy(coef_hbm, coef, coef_sem)
    coef_copy.start()
    leg_copies = [pltpu.make_async_copy(leg_hbm.at[:, jt], leg.at[jt], leg_sem.at[jt]) for jt in range(8)]

    barrier = pltpu.get_barrier_semaphore()

    def signal(sem):
        for offset in near:
            pl.semaphore_signal(sem, inc=1, device_id={"blk": at(*offset)}, device_id_type=MESH)

    signal(barrier)

    orders_copy.wait()
    for h in range(2):
        order_cols[h * 128 : (h + 1) * 128, :] = jnp.broadcast_to(orders_v[h : h + 1, :], (128, 128)).T
    cycles_copy.wait()
    lanes = lax.broadcasted_iota(I32, (128, 128), 1)

    def pick(ib, carry):
        wanted = jnp.broadcast_to(cycles[pl.ds(ib, 1), :], (128, 128)).T
        row = pl.multiple_of(ib * 128, 128)
        for jb in range(8):
            onehot[pl.ds(row, 128), jb * 128 : (jb + 1) * 128] = jnp.where(
                wanted == lanes + jb * 128, 1.0, 0.0
            ).astype(BF16)
        return carry

    lax.fori_loop(0, 8, pick, 0)

    coef_copy.wait()
    for copy in leg_copies[:4]:
        copy.start()
    packed = coef[...].reshape(2 * ROWS, 128).T
    column = lax.broadcasted_iota(I32, (1, 2 * ROWS), 1)
    row_id, pair_id = column >> 1, column & 1
    for p in range(2):
        order = order_cols[pl.ds(me * 2 + p, 1), :][:, :1]
        lower = jnp.where(row_id < DEGREE + 1 - order, 1, 0)
        parity_of = jnp.where(pair_id == p, (lower + order + 1) & 1, 2)
        for parity in range(2):
            keep = jnp.where(parity_of == parity, 1.0, 0.0).astype(BF16)
            for part in range(2):
                row = ((p * 2 + part) * 2 + parity) * 64
                stacked[row : row + 64, :] = packed[part * 64 : (part + 1) * 64] * keep

    pl.semaphore_wait(barrier, 10)
    signal(ring_sems.at[0])
    for copy in leg_copies[4:]:
        copy.start()

    def legs(jp, carry):
        for jt in range(2):
            pltpu.make_async_copy(leg_hbm.at[:, 2 * jp + jt], leg.at[2 * jp + jt], leg_sem.at[2 * jp + jt]).wait()
        table = jnp.concatenate(
            [leg[2 * jp].reshape(2 * ROWS, 128), leg[2 * jp + 1].reshape(2 * ROWS, 128)], axis=1
        )
        spec[:, pl.ds(pl.multiple_of(jp * 256, 256), 256)] = jnp.dot(
            stacked[...], table, preferred_element_type=F32
        ).astype(BF16)
        return carry

    lax.fori_loop(0, 3, legs, 0)
    pl.semaphore_wait(ring_sems.at[0], 10)
    signal(ring_sems.at[1])
    lax.fori_loop(3, 4, legs, 0)

    def choose(ib, carry):
        row = pl.multiple_of(ib * 256, 256)
        outbox[pl.ds(pl.multiple_of(ib * 32, 32), 32)] = (
            lax.dot_general(
                onehot[pl.ds(row, 256), :], spec[...], (((1,), (1,)), ((), ())), preferred_element_type=F32
            )
            .reshape(32, 8, COLS)
            .astype(BF16)
        )
        return carry

    lax.fori_loop(0, 4, choose, 0)

    def send(dz, dy, dx, dc):
        target = at(dz, dy, dx, dc)
        pltpu.make_async_remote_copy(
            src_ref=outbox.at[target], dst_ref=inbox.at[me], send_sem=send_sem, recv_sem=recv_sem.at[dz],
            device_id={"blk": target}, device_id_type=MESH,
        ).start()

    def send_all(planes, axes, flip):
        count = 3 ** len(axes)

        def one(t, carry):
            offset = [0, 0, 0, flip]
            rest = t
            for axis in axes:
                offset[axis] = rest % 3 + 1
                rest = rest // 3
            for dz in planes:
                send(dz, *offset[1:])
            return carry

        if count == 1:
            one(0, 0)
        else:
            lax.fori_loop(0, count, one, 0)

    across = (2, 1, 3)
    send_all(across, (), 0)
    send_all((2, 1, 3, 0), (2,), 0)
    send_all((2, 1, 3, 0), (1,), 0)
    send_all((2, 1, 3, 0), (), 1)
    for axes, flip in (((1, 2), 0), ((1,), 1), ((2,), 1)):
        send_all((0,), axes, flip)
    pl.semaphore_wait(ring_sems.at[1], 10)
    signal(ring_sems.at[2])
    for axes, flip in (((1, 2), 0), ((1,), 1), ((2,), 1)):
        send_all((2,), axes, flip)
    send_all((0,), (1, 2), 1)
    pl.semaphore_wait(ring_sems.at[2], 10)
    send_all((2,), (1, 2), 1)
    for axes, flip in (((1, 2), 0), ((1,), 1), ((2,), 1), ((1, 2), 1)):
        send_all((1, 3), axes, flip)
    inbox[me] = outbox[me]

    place = me % PLANE
    is_even = lax.broadcasted_iota(I32, (1, 128), 1) < FIELDS
    energy = jnp.zeros((1, 128), F32)
    for p in range(2):
        order = order_cols[pl.ds(me * 2 + p, 1), :]
        has_zero = jnp.where(order % 2 == 1, DEGREE - order, order) == 0
        for part in range(2):
            row = (p * 2 + part) * 128
            squares = jnp.zeros((128, 128), F32)
            for jb in range(8):
                values = spec[row : row + 128, jb * 128 : (jb + 1) * 128].astype(F32)
                squares = squares + values * values
            weight = jnp.where(is_even, jnp.where(has_zero, 1.0 - part, 2.0), 2.0)
            energy = energy + weight * jnp.sum(squares.T, axis=0, keepdims=True)
    e_mine[0] = energy
    e_plane[place] = energy

    def back_of(slot):
        late = slot // 2
        swap = (slot % 2 + z + 1) % 2
        return (1 - late) * 2 * slot + late * (1 + 2 * swap)

    lane = lax.broadcasted_iota(I32, (16, 128), 1)

    def basis_step(step, carry):
        slot, sub = step // 2, step % 2
        first = (z + 4 - back_of(slot)) % 4 * 64 + sub * 32
        for p in range(2):
            order = order_cols[pl.ds(first + p, 16, stride=2), :]
            even = jnp.where((order & 1) == 1, DEGREE - order, order)
            for parity in range(2):
                m = even if parity == 0 else DEGREE - even
                cosine, sine = sincos(m * lane)
                turn_cos, turn_sin = sincos(m * 128)
                factor = jnp.where(m == 0, 1.0, 2.0)
                re, im = factor * cosine, -factor * sine
                row = pl.multiple_of(parity * COLS + slot * 128 + p * 64 + sub * 16, 16)
                for a in range(HALF // 128):
                    basis[pl.ds(row, 16), a * 128 : (a + 1) * 128] = re.astype(BF16)
                    basis[pl.ds(row + 32, 16), a * 128 : (a + 1) * 128] = im.astype(BF16)
                    re, im = re * turn_cos + im * turn_sin, im * turn_cos - re * turn_sin
        return carry

    lax.fori_loop(0, 8, basis_step, 0)

    def tell(t, carry):
        target = at(0, t // 8, (t // 2) % 4, t % 2)
        pltpu.make_async_remote_copy(
            src_ref=e_mine.at[0], dst_ref=e_plane.at[place], send_sem=e_sems.at[0], recv_sem=e_sems.at[1],
            device_id={"blk": target}, device_id_type=MESH,
        ).start()
        return carry

    lax.fori_loop(1, PLANE, tell, 0)

    def landed(back, count):
        pltpu.make_async_remote_copy(
            src_ref=outbox.at[pl.ds(0, count)], dst_ref=inbox.at[pl.ds(0, count)],
            send_sem=send_sem, recv_sem=recv_sem.at[back], device_id={"blk": at(0, 0, 0, 1)}, device_id_type=MESH,
        ).wait_recv()

    def build(slot, even_to, odd_to):
        back = back_of(slot)
        plane = (z + 4 - back) % 4
        @pl.when(slot == 0)
        def _():
            landed(0, PLANE - 1)

        @pl.when(slot > 0)
        def _():
            landed(back, PLANE)

        for g in range(4):
            wide[g] = inbox[pl.ds(plane * PLANE, PLANE), :, g * 128 : (g + 1) * 128].astype(F32).reshape(256, 128)
        col = pl.multiple_of(slot % 2 * 128, 128)
        for i in range(8):
            block = jnp.concatenate([wide[g, pl.ds(i, PLANE, stride=8), :] for g in range(4)], axis=0)
            block = block.T.astype(BF16)
            even_to[i * 64 : (i + 1) * 64, pl.ds(col, 128)] = block[:64]
            odd_to[i * 64 : (i + 1) * 64, pl.ds(col, 128)] = block[64:]

    def build_first(slot, carry):
        build(slot, first_x.at[0], first_x.at[1])
        return carry

    def build_last(slot, carry):
        build(slot, even_x, odd_x)
        return carry

    def sum_first(n, carry):
        cols = pl.ds(pl.multiple_of(n * 256, 256), 256)
        evens[:, cols] = jnp.dot(first_x[0], basis[:256, cols], preferred_element_type=F32)
        odds[:, cols] = jnp.dot(first_x[1], basis[COLS : COLS + 256, cols], preferred_element_type=F32)
        return carry

    lax.fori_loop(0, 2, build_first, 0)
    told = pltpu.make_async_remote_copy(
        src_ref=e_plane.at[pl.ds(0, PLANE - 1)], dst_ref=e_plane.at[pl.ds(0, PLANE - 1)],
        send_sem=e_sems.at[0], recv_sem=e_sems.at[1], device_id={"blk": at(0, 0, 0, 1)}, device_id_type=MESH,
    )
    told.wait_send()
    told.wait_recv()
    total = e_plane[0]
    for s in range(1, PLANE):
        total = total + e_plane[s]
    e_mine[1] = total
    e_all[z] = total
    lax.fori_loop(0, 8, sum_first, 0)

    for d in range(1, 4):
        pltpu.make_async_remote_copy(
            src_ref=e_mine.at[1], dst_ref=e_all.at[z], send_sem=e_sems.at[2], recv_sem=e_sems.at[3],
            device_id={"blk": at(d, 0, 0, 0)}, device_id_type=MESH,
        ).start()

    lax.fori_loop(2, 4, build_last, 0)

    told = pltpu.make_async_remote_copy(
        src_ref=e_all.at[pl.ds(0, 3)], dst_ref=e_all.at[pl.ds(0, 3)],
        send_sem=e_sems.at[2], recv_sem=e_sems.at[3], device_id={"blk": at(0, 0, 0, 1)}, device_id_type=MESH,
    )
    told.wait_send()
    told.wait_recv()
    energy_ref[...] = (e_all[0] + e_all[1]) + (e_all[2] + e_all[3])
    sent = pltpu.make_async_remote_copy(
        src_ref=outbox.at[pl.ds(0, NBLK - 1)], dst_ref=inbox.at[pl.ds(0, NBLK - 1)],
        send_sem=send_sem, recv_sem=recv_sem.at[0], device_id={"blk": at(0, 0, 0, 1)}, device_id_type=MESH,
    )
    sent.wait_send()


def synthesize(energy_in, even_x, odd_x, basis, evens, odds, potential_hbm, energy_ref, tile, tile_sems):
    both = energy_in[...]
    energy_ref[...] = (both[:, :FIELDS] + both[:, FIELDS:]) * (1.0 / NLAT)
    steps = HALF // 256
    copies = []
    for n in range(steps):
        cols = slice(n * 256, (n + 1) * 256)
        even = evens[:, cols] + jnp.dot(even_x[...], basis[256:COLS, cols], preferred_element_type=F32)
        odd = odds[:, cols] + jnp.dot(odd_x[...], basis[COLS + 256 :, cols], preferred_element_type=F32)
        for half in range(2):
            tile[n, half] = (even + odd if half == 0 else even - odd).astype(BF16).reshape(8, FIELDS, 256)
            copy = pltpu.make_async_copy(
                tile.at[n, half], potential_hbm.at[:, :, pl.ds(half * HALF + n * 256, 256)], tile_sems.at[n, half]
            )
            copy.start()
            copies.append(copy)
    for copy in copies:
        copy.wait()


def shards(load_coef, legendre, slab_orders, cycle_rows):
    any_space = pl.BlockSpec(memory_space=pl.ANY)
    vmem = pl.BlockSpec(memory_space=pltpu.VMEM)
    coef = load_coef.transpose(1, 0, 2)
    table = legendre.transpose(1, 0, 2).reshape(ROWS, 2, 8, 128).transpose(0, 2, 1, 3)
    even_x, odd_x, basis, evens, odds, energy = pl.pallas_call(
        exchange,
        out_shape=(
            jax.ShapeDtypeStruct((COLS, 256), BF16),
            jax.ShapeDtypeStruct((COLS, 256), BF16),
            jax.ShapeDtypeStruct((2 * COLS, HALF), BF16),
            jax.ShapeDtypeStruct((COLS, HALF), F32),
            jax.ShapeDtypeStruct((COLS, HALF), F32),
            jax.ShapeDtypeStruct((1, 128), F32),
        ),
        in_specs=[pl.BlockSpec(memory_space=pltpu.HBM)] * 4,
        out_specs=(vmem,) * 6,
        scratch_shapes=[
            pltpu.VMEM((2, 128), I32),
            pltpu.VMEM((8, 128), I32),
            pltpu.VMEM((ROWS, 2, 128), BF16),
            pltpu.VMEM((8, ROWS, 2, 128), BF16),
            pltpu.VMEM((2, COLS, 256), BF16),
            pltpu.VMEM((COLS, 2 * ROWS), BF16),
            pltpu.VMEM((COLS, NLAT), BF16),
            pltpu.VMEM((NLAT, NLAT), BF16),
            pltpu.VMEM((NBLK, 8, COLS), BF16),
            pltpu.VMEM((NBLK, 8, COLS), BF16),
            pltpu.VMEM((4, 256, 128), F32),
            pltpu.VMEM((256, 128), I32),
            pltpu.VMEM((2, 1, 128), F32),
            pltpu.VMEM((PLANE, 1, 128), F32),
            pltpu.VMEM((4, 1, 128), F32),
            pltpu.SemaphoreType.DMA((2,)),
            pltpu.SemaphoreType.DMA,
            pltpu.SemaphoreType.DMA((8,)),
            pltpu.SemaphoreType.DMA,
            pltpu.SemaphoreType.DMA((4,)),
            pltpu.SemaphoreType.DMA((4,)),
            pltpu.SemaphoreType.REGULAR((3,)),
        ],
        compiler_params=pltpu.CompilerParams(
            collective_id=0, has_side_effects=True, vmem_limit_bytes=36 * 1024 * 1024
        ),
        name="exchange",
    )(*[pltpu.with_memory_space_constraint(a, pltpu.HBM) for a in (slab_orders.reshape(2, 128), cycle_rows.reshape(8, 128), coef, table)])
    potential, energy = pl.pallas_call(
        synthesize,
        out_shape=(
            jax.ShapeDtypeStruct((8, FIELDS, NLON), BF16),
            jax.ShapeDtypeStruct((1, FIELDS), F32),
        ),
        in_specs=[vmem] * 6,
        out_specs=(any_space, vmem),
        scratch_shapes=[
            pltpu.VMEM((8, 2, 8, FIELDS, 256), BF16),
            pltpu.SemaphoreType.DMA((8, 2)),
        ],
        compiler_params=pltpu.CompilerParams(vmem_limit_bytes=20 * 1024 * 1024),
        name="synthesize",
    )(energy, even_x, odd_x, basis, evens, odds)
    return potential, energy.reshape(FIELDS)


def solution(mesh):
    in_specs = (P("blk", None, "rep"), P("blk", None, None), P(), P())
    out_specs = (P("blk", "rep", None), P("rep"))
    return jax.shard_map(shards, mesh=mesh, in_specs=in_specs, out_specs=out_specs, check_vma=False)
```

```python
import math

import jax
import jax.numpy as jnp
from jax import lax
from jax.experimental import pallas as pl
from jax.experimental.pallas import tpu as pltpu
from jax.sharding import PartitionSpec as P

BF16 = jnp.bfloat16
F32 = jnp.float32
I32 = jnp.int32
MESH = pl.DeviceIdType.MESH
NLON = 4096
HALF = NLON // 2
DEGREE = 2047
ROWS = 2049
NLAT = 1024
FIELDS = 64
NBLK = 128
PLANE = 32
COLS = 512


def sincos(phase):
    turned = (phase + 512) & 4095
    quadrant = turned >> 10
    theta = ((turned & 1023) - 512).astype(F32) * (2.0 * math.pi / NLON)
    t2 = theta * theta
    s = theta * (1.0 + t2 * (-1.0 / 6 + t2 * (1.0 / 120 + t2 * (-1.0 / 5040 + t2 * (1.0 / 362880)))))
    c = 1.0 + t2 * (-0.5 + t2 * (1.0 / 24 + t2 * (-1.0 / 720 + t2 * (1.0 / 40320))))
    odd = (quadrant & 1) == 1
    cosine = jnp.where(odd, s, c)
    sine = jnp.where(odd, c, s)
    flip_cos = ((quadrant + 1) & 2) == 2
    flip_sin = (quadrant & 2) == 2
    return jnp.where(flip_cos, -cosine, cosine), jnp.where(flip_sin, -sine, sine)


def exchange(
    orders_hbm, cycles_hbm, coef_hbm, leg_hbm,
    even_x, odd_x, basis, evens, odds, energy_ref,
    orders_v, cycles, coef, leg, first_x, stacked, spec, onehot, outbox, inbox, wide, order_cols, e_mine, e_plane, e_all,
    small_sems, coef_sem, leg_sem, send_sem, recv_sem, e_sems, ring_sems,
):
    me = lax.axis_index("blk")
    z, y, x, c = me // 32, (me // 8) % 4, (me // 2) % 4, me % 2

    def at(dz, dy, dx, dc):
        return (((z + dz) % 4 * 4 + (y + dy) % 4) * 4 + (x + dx) % 4) * 2 + (c + dc) % 2

    near = [(d, 0, 0, 0) for d in (1, 2, 3)] + [(0, d, 0, 0) for d in (1, 2, 3)]
    near += [(0, 0, d, 0) for d in (1, 2, 3)] + [(0, 0, 0, 1)]

    orders_copy = pltpu.make_async_copy(orders_hbm, orders_v, small_sems.at[0])
    orders_copy.start()
    cycles_copy = pltpu.make_async_copy(cycles_hbm, cycles, small_sems.at[1])
    cycles_copy.start()
    coef_copy = pltpu.make_async_copy(coef_hbm, coef, coef_sem)
    coef_copy.start()
    leg_copies = [pltpu.make_async_copy(leg_hbm.at[:, jt], leg.at[jt], leg_sem.at[jt]) for jt in range(8)]

    barrier = pltpu.get_barrier_semaphore()

    def signal(sem):
        for offset in near:
            pl.semaphore_signal(sem, inc=1, device_id={"blk": at(*offset)}, device_id_type=MESH)

    signal(barrier)

    orders_copy.wait()
    for h in range(2):
        order_cols[h * 128 : (h + 1) * 128, :] = jnp.broadcast_to(orders_v[h : h + 1, :], (128, 128)).T
    cycles_copy.wait()
    lanes = lax.broadcasted_iota(I32, (128, 128), 1)

    def pick(ib, carry):
        wanted = jnp.broadcast_to(cycles[pl.ds(ib, 1), :], (128, 128)).T
        row = pl.multiple_of(ib * 128, 128)
        for jb in range(8):
            onehot[pl.ds(row, 128), jb * 128 : (jb + 1) * 128] = jnp.where(
                wanted == lanes + jb * 128, 1.0, 0.0
            ).astype(BF16)
        return carry

    lax.fori_loop(0, 8, pick, 0)

    coef_copy.wait()
    for copy in leg_copies[:4]:
        copy.start()
    packed = coef[...].reshape(2 * ROWS, 128).T
    column = lax.broadcasted_iota(I32, (1, 2 * ROWS), 1)
    row_id, pair_id = column >> 1, column & 1
    for p in range(2):
        order = order_cols[pl.ds(me * 2 + p, 1), :][:, :1]
        lower = jnp.where(row_id < DEGREE + 1 - order, 1, 0)
        parity_of = jnp.where(pair_id == p, (lower + order + 1) & 1, 2)
        for parity in range(2):
            keep = jnp.where(parity_of == parity, 1.0, 0.0).astype(BF16)
            for part in range(2):
                row = ((p * 2 + part) * 2 + parity) * 64
                stacked[row : row + 64, :] = packed[part * 64 : (part + 1) * 64] * keep

    pl.semaphore_wait(barrier, 10)
    signal(ring_sems.at[0])
    for copy in leg_copies[4:]:
        copy.start()

    def legs(jp, carry):
        for jt in range(2):
            pltpu.make_async_copy(leg_hbm.at[:, 2 * jp + jt], leg.at[2 * jp + jt], leg_sem.at[2 * jp + jt]).wait()
        table = jnp.concatenate(
            [leg[2 * jp].reshape(2 * ROWS, 128), leg[2 * jp + 1].reshape(2 * ROWS, 128)], axis=1
        )
        spec[:, pl.ds(pl.multiple_of(jp * 256, 256), 256)] = jnp.dot(
            stacked[...], table, preferred_element_type=F32
        ).astype(BF16)
        return carry

    lax.fori_loop(0, 3, legs, 0)
    pl.semaphore_wait(ring_sems.at[0], 10)
    signal(ring_sems.at[1])
    lax.fori_loop(3, 4, legs, 0)

    def choose(ib, carry):
        row = pl.multiple_of(ib * 256, 256)
        outbox[pl.ds(pl.multiple_of(ib * 32, 32), 32)] = (
            lax.dot_general(
                onehot[pl.ds(row, 256), :], spec[...], (((1,), (1,)), ((), ())), preferred_element_type=F32
            )
            .reshape(32, 8, COLS)
            .astype(BF16)
        )
        return carry

    lax.fori_loop(0, 4, choose, 0)

    def send(dz, dy, dx, dc):
        target = at(dz, dy, dx, dc)
        pltpu.make_async_remote_copy(
            src_ref=outbox.at[target], dst_ref=inbox.at[me], send_sem=send_sem, recv_sem=recv_sem.at[dz],
            device_id={"blk": target}, device_id_type=MESH,
        ).start()

    def send_all(planes, axes, flip):
        count = 3 ** len(axes)

        def one(t, carry):
            offset = [0, 0, 0, flip]
            rest = t
            for axis in axes:
                offset[axis] = rest % 3 + 1
                rest = rest // 3
            for dz in planes:
                send(dz, *offset[1:])
            return carry

        if count == 1:
            one(0, 0)
        else:
            lax.fori_loop(0, count, one, 0)

    beside = 1 + 2 * (z % 2)
    across = 4 - beside
    send_all((beside, 0, across), (2,), 0)
    send_all((beside, 0, across), (1,), 0)
    send_all((beside, 0, across), (), 1)
    send_all((beside, across), (), 0)
    send_all((0,), (1, 2), 0)
    send_all((0,), (1,), 1)
    send_all((0,), (2,), 1)

    place = me % PLANE
    is_even = lax.broadcasted_iota(I32, (1, 128), 1) < FIELDS
    energy = jnp.zeros((1, 128), F32)
    for p in range(2):
        order = order_cols[pl.ds(me * 2 + p, 1), :]
        has_zero = jnp.where(order % 2 == 1, DEGREE - order, order) == 0
        for part in range(2):
            row = (p * 2 + part) * 128
            squares = jnp.zeros((128, 128), F32)
            for jb in range(8):
                values = spec[row : row + 128, jb * 128 : (jb + 1) * 128].astype(F32)
                squares = squares + values * values
            weight = jnp.where(is_even, jnp.where(has_zero, 1.0 - part, 2.0), 2.0)
            energy = energy + weight * jnp.sum(squares.T, axis=0, keepdims=True)
    e_mine[0] = energy
    e_all[z] = energy
    pl.semaphore_wait(ring_sems.at[1], 10)
    signal(ring_sems.at[2])
    for axes, flip in (((1, 2), 0), ((1,), 1), ((2,), 1)):
        send_all((beside, across), axes, flip)
    send_all((0,), (1, 2), 1)

    for d in range(1, 4):
        pltpu.make_async_remote_copy(
            src_ref=e_mine.at[0], dst_ref=e_all.at[z], send_sem=e_sems.at[2], recv_sem=e_sems.at[3],
            device_id={"blk": at(d, 0, 0, 0)}, device_id_type=MESH,
        ).start()
    pl.semaphore_wait(ring_sems.at[2], 10)
    send_all((beside, across), (1, 2), 1)
    for axes, flip in (((), 0), ((2,), 0), ((1,), 0), ((), 1), ((1, 2), 0), ((1,), 1), ((2,), 1), ((1, 2), 1)):
        send_all((2,), axes, flip)
    inbox[me] = outbox[me]


    def back_of(slot):
        return slot % 2 * across * (1 - slot // 2) + slot // 2 * (beside + slot % 2 * (2 - beside))

    lane = lax.broadcasted_iota(I32, (16, 128), 1)

    def basis_step(step, carry):
        slot, sub = step // 2, step % 2
        first = (z + 4 - back_of(slot)) % 4 * 64 + sub * 32
        for p in range(2):
            order = order_cols[pl.ds(first + p, 16, stride=2), :]
            even = jnp.where((order & 1) == 1, DEGREE - order, order)
            for parity in range(2):
                m = even if parity == 0 else DEGREE - even
                cosine, sine = sincos(m * lane)
                turn_cos, turn_sin = sincos(m * 128)
                factor = jnp.where(m == 0, 1.0, 2.0)
                re, im = factor * cosine, -factor * sine
                row = pl.multiple_of(parity * COLS + slot * 128 + p * 64 + sub * 16, 16)
                for a in range(HALF // 128):
                    basis[pl.ds(row, 16), a * 128 : (a + 1) * 128] = re.astype(BF16)
                    basis[pl.ds(row + 32, 16), a * 128 : (a + 1) * 128] = im.astype(BF16)
                    re, im = re * turn_cos + im * turn_sin, im * turn_cos - re * turn_sin
        return carry

    lax.fori_loop(0, 8, basis_step, 0)

    def landed(back, count):
        pltpu.make_async_remote_copy(
            src_ref=outbox.at[pl.ds(0, count)], dst_ref=inbox.at[pl.ds(0, count)],
            send_sem=send_sem, recv_sem=recv_sem.at[back], device_id={"blk": at(0, 0, 0, 1)}, device_id_type=MESH,
        ).wait_recv()

    def build(slot, even_to, odd_to, col):
        plane = (z + 4 - back_of(slot)) % 4
        for g in range(4):
            wide[g] = inbox[pl.ds(plane * PLANE, PLANE), :, g * 128 : (g + 1) * 128].astype(F32).reshape(256, 128)
        for i in range(8):
            block = jnp.concatenate([wide[g, pl.ds(i, PLANE, stride=8), :] for g in range(4)], axis=0)
            block = block.T.astype(BF16)
            even_to[i * 64 : (i + 1) * 64, pl.ds(col, 128)] = block[:64]
            odd_to[i * 64 : (i + 1) * 64, pl.ds(col, 128)] = block[64:]

    def build_first(slot, carry):
        @pl.when(slot == 0)
        def _():
            landed(0, PLANE - 1)

        @pl.when(slot > 0)
        def _():
            landed(back_of(slot), PLANE)

        build(slot, first_x.at[0], first_x.at[1], pl.multiple_of(slot * 128, 128))
        return carry

    def sum_first(n, carry):
        cols = pl.ds(pl.multiple_of(n * 256, 256), 256)
        evens[:, cols] = jnp.dot(first_x[0], basis[:384, cols], preferred_element_type=F32)
        odds[:, cols] = jnp.dot(first_x[1], basis[COLS : COLS + 384, cols], preferred_element_type=F32)
        return carry

    told = pltpu.make_async_remote_copy(
        src_ref=e_all.at[pl.ds(0, 3)], dst_ref=e_all.at[pl.ds(0, 3)],
        send_sem=e_sems.at[2], recv_sem=e_sems.at[3], device_id={"blk": at(0, 0, 0, 1)}, device_id_type=MESH,
    )
    told.wait_send()
    told.wait_recv()
    column_sum = (e_all[0] + e_all[1]) + (e_all[2] + e_all[3])
    e_mine[1] = column_sum
    e_plane[place] = column_sum
    lax.fori_loop(0, 1, build_first, 0)

    def tell(t, carry):
        target = at(0, t // 8, (t // 2) % 4, t % 2)
        pltpu.make_async_remote_copy(
            src_ref=e_mine.at[1], dst_ref=e_plane.at[place], send_sem=e_sems.at[0], recv_sem=e_sems.at[1],
            device_id={"blk": target}, device_id_type=MESH,
        ).start()
        return carry

    lax.fori_loop(1, PLANE, tell, 0)
    lax.fori_loop(1, 3, build_first, 0)
    lax.fori_loop(0, 8, sum_first, 0)
    told = pltpu.make_async_remote_copy(
        src_ref=e_plane.at[pl.ds(0, PLANE - 1)], dst_ref=e_plane.at[pl.ds(0, PLANE - 1)],
        send_sem=e_sems.at[0], recv_sem=e_sems.at[1], device_id={"blk": at(0, 0, 0, 1)}, device_id_type=MESH,
    )
    told.wait_send()
    told.wait_recv()
    total = e_plane[0]
    for s in range(1, PLANE):
        total = total + e_plane[s]
    energy_ref[...] = total

    landed(2, PLANE)
    build(3, even_x, odd_x, 0)
    sent = pltpu.make_async_remote_copy(
        src_ref=outbox.at[pl.ds(0, NBLK - 1)], dst_ref=inbox.at[pl.ds(0, NBLK - 1)],
        send_sem=send_sem, recv_sem=recv_sem.at[0], device_id={"blk": at(0, 0, 0, 1)}, device_id_type=MESH,
    )
    sent.wait_send()


def synthesize(energy_in, even_x, odd_x, basis, evens, odds, potential_hbm, energy_ref, tile, tile_sems):
    both = energy_in[...]
    energy_ref[...] = (both[:, :FIELDS] + both[:, FIELDS:]) * (1.0 / NLAT)
    steps = HALF // 256
    copies = []
    for n in range(steps):
        cols = slice(n * 256, (n + 1) * 256)
        even = evens[:, cols] + jnp.dot(even_x[...], basis[384:COLS, cols], preferred_element_type=F32)
        odd = odds[:, cols] + jnp.dot(odd_x[...], basis[COLS + 384 :, cols], preferred_element_type=F32)
        for half in range(2):
            tile[n, half] = (even + odd if half == 0 else even - odd).astype(BF16).reshape(8, FIELDS, 256)
            copy = pltpu.make_async_copy(
                tile.at[n, half], potential_hbm.at[:, :, pl.ds(half * HALF + n * 256, 256)], tile_sems.at[n, half]
            )
            copy.start()
            copies.append(copy)
    for copy in copies:
        copy.wait()


def shards(load_coef, legendre, slab_orders, cycle_rows):
    any_space = pl.BlockSpec(memory_space=pl.ANY)
    vmem = pl.BlockSpec(memory_space=pltpu.VMEM)
    coef = load_coef.transpose(1, 0, 2)
    table = legendre.transpose(1, 0, 2).reshape(ROWS, 2, 8, 128).transpose(0, 2, 1, 3)
    even_x, odd_x, basis, evens, odds, energy = pl.pallas_call(
        exchange,
        out_shape=(
            jax.ShapeDtypeStruct((COLS, 128), BF16),
            jax.ShapeDtypeStruct((COLS, 128), BF16),
            jax.ShapeDtypeStruct((2 * COLS, HALF), BF16),
            jax.ShapeDtypeStruct((COLS, HALF), F32),
            jax.ShapeDtypeStruct((COLS, HALF), F32),
            jax.ShapeDtypeStruct((1, 128), F32),
        ),
        in_specs=[pl.BlockSpec(memory_space=pltpu.HBM)] * 4,
        out_specs=(vmem,) * 6,
        scratch_shapes=[
            pltpu.VMEM((2, 128), I32),
            pltpu.VMEM((8, 128), I32),
            pltpu.VMEM((ROWS, 2, 128), BF16),
            pltpu.VMEM((8, ROWS, 2, 128), BF16),
            pltpu.VMEM((2, COLS, 384), BF16),
            pltpu.VMEM((COLS, 2 * ROWS), BF16),
            pltpu.VMEM((COLS, NLAT), BF16),
            pltpu.VMEM((NLAT, NLAT), BF16),
            pltpu.VMEM((NBLK, 8, COLS), BF16),
            pltpu.VMEM((NBLK, 8, COLS), BF16),
            pltpu.VMEM((4, 256, 128), F32),
            pltpu.VMEM((256, 128), I32),
            pltpu.VMEM((2, 1, 128), F32),
            pltpu.VMEM((PLANE, 1, 128), F32),
            pltpu.VMEM((4, 1, 128), F32),
            pltpu.SemaphoreType.DMA((2,)),
            pltpu.SemaphoreType.DMA,
            pltpu.SemaphoreType.DMA((8,)),
            pltpu.SemaphoreType.DMA,
            pltpu.SemaphoreType.DMA((4,)),
            pltpu.SemaphoreType.DMA((4,)),
            pltpu.SemaphoreType.REGULAR((3,)),
        ],
        compiler_params=pltpu.CompilerParams(
            collective_id=0, has_side_effects=True, vmem_limit_bytes=36 * 1024 * 1024
        ),
        name="exchange",
    )(*[pltpu.with_memory_space_constraint(a, pltpu.HBM) for a in (slab_orders.reshape(2, 128), cycle_rows.reshape(8, 128), coef, table)])
    potential, energy = pl.pallas_call(
        synthesize,
        out_shape=(
            jax.ShapeDtypeStruct((8, FIELDS, NLON), BF16),
            jax.ShapeDtypeStruct((1, FIELDS), F32),
        ),
        in_specs=[vmem] * 6,
        out_specs=(any_space, vmem),
        scratch_shapes=[
            pltpu.VMEM((8, 2, 8, FIELDS, 256), BF16),
            pltpu.SemaphoreType.DMA((8, 2)),
        ],
        compiler_params=pltpu.CompilerParams(vmem_limit_bytes=20 * 1024 * 1024),
        name="synthesize",
    )(energy, even_x, odd_x, basis, evens, odds)
    return potential, energy.reshape(FIELDS)


def solution(mesh):
    in_specs = (P("blk", None, "rep"), P("blk", None, None), P(), P())
    out_specs = (P("blk", "rep", None), P("rep"))
    return jax.shard_map(shards, mesh=mesh, in_specs=in_specs, out_specs=out_specs, check_vma=False)
```

```python
import math

import jax
import jax.numpy as jnp
from jax import lax
from jax.experimental import pallas as pl
from jax.experimental.pallas import tpu as pltpu
from jax.sharding import PartitionSpec as P

BF16 = jnp.bfloat16
F32 = jnp.float32
I32 = jnp.int32
MESH = pl.DeviceIdType.MESH
NLON = 4096
HALF = NLON // 2
DEGREE = 2047
ROWS = 2049
NLAT = 1024
FIELDS = 64
NBLK = 128
PLANE = 32
COLS = 512


def sincos(phase):
    turned = (phase + 512) & 4095
    quadrant = turned >> 10
    theta = ((turned & 1023) - 512).astype(F32) * (2.0 * math.pi / NLON)
    t2 = theta * theta
    s = theta * (1.0 + t2 * (-1.0 / 6 + t2 * (1.0 / 120 + t2 * (-1.0 / 5040 + t2 * (1.0 / 362880)))))
    c = 1.0 + t2 * (-0.5 + t2 * (1.0 / 24 + t2 * (-1.0 / 720 + t2 * (1.0 / 40320))))
    odd = (quadrant & 1) == 1
    cosine = jnp.where(odd, s, c)
    sine = jnp.where(odd, c, s)
    flip_cos = ((quadrant + 1) & 2) == 2
    flip_sin = (quadrant & 2) == 2
    return jnp.where(flip_cos, -cosine, cosine), jnp.where(flip_sin, -sine, sine)


def exchange(
    orders_hbm, cycles_hbm, coef_hbm, leg_hbm,
    even_x, odd_x, basis, evens, odds, energy_ref,
    orders_v, cycles, coef, leg, first_x, stacked, spec, onehot, outbox, inbox, wide, order_cols, e_mine, e_plane, e_all,
    small_sems, coef_sem, leg_sem, send_sem, recv_sem, e_sems, ring_sems,
):
    me = lax.axis_index("blk")
    z, y, x, c = me // 32, (me // 8) % 4, (me // 2) % 4, me % 2

    def at(dz, dy, dx, dc):
        return (((z + dz) % 4 * 4 + (y + dy) % 4) * 4 + (x + dx) % 4) * 2 + (c + dc) % 2

    near = [(d, 0, 0, 0) for d in (1, 2, 3)] + [(0, d, 0, 0) for d in (1, 2, 3)]
    near += [(0, 0, d, 0) for d in (1, 2, 3)] + [(0, 0, 0, 1)]

    orders_copy = pltpu.make_async_copy(orders_hbm, orders_v, small_sems.at[0])
    orders_copy.start()
    cycles_copy = pltpu.make_async_copy(cycles_hbm, cycles, small_sems.at[1])
    cycles_copy.start()
    coef_copy = pltpu.make_async_copy(coef_hbm, coef, coef_sem)
    coef_copy.start()
    leg_copies = [pltpu.make_async_copy(leg_hbm.at[:, jt], leg.at[jt], leg_sem.at[jt]) for jt in range(8)]

    barrier = pltpu.get_barrier_semaphore()

    def signal(sem):
        for offset in near:
            pl.semaphore_signal(sem, inc=1, device_id={"blk": at(*offset)}, device_id_type=MESH)

    signal(barrier)

    orders_copy.wait()
    for h in range(2):
        order_cols[h * 128 : (h + 1) * 128, :] = jnp.broadcast_to(orders_v[h : h + 1, :], (128, 128)).T
    cycles_copy.wait()
    lanes = lax.broadcasted_iota(I32, (128, 128), 1)

    def pick(ib, carry):
        wanted = jnp.broadcast_to(cycles[pl.ds(ib, 1), :], (128, 128)).T
        row = pl.multiple_of(ib * 128, 128)
        for jb in range(8):
            onehot[pl.ds(row, 128), jb * 128 : (jb + 1) * 128] = jnp.where(
                wanted == lanes + jb * 128, 1.0, 0.0
            ).astype(BF16)
        return carry

    lax.fori_loop(0, 8, pick, 0)

    coef_copy.wait()
    for copy in leg_copies[:4]:
        copy.start()
    packed = coef[...].reshape(2 * ROWS, 128).T
    column = lax.broadcasted_iota(I32, (1, 2 * ROWS), 1)
    row_id, pair_id = column >> 1, column & 1
    for p in range(2):
        order = order_cols[pl.ds(me * 2 + p, 1), :][:, :1]
        lower = jnp.where(row_id < DEGREE + 1 - order, 1, 0)
        parity_of = jnp.where(pair_id == p, (lower + order + 1) & 1, 2)
        for parity in range(2):
            keep = jnp.where(parity_of == parity, 1.0, 0.0).astype(BF16)
            for part in range(2):
                row = ((p * 2 + part) * 2 + parity) * 64
                stacked[row : row + 64, :] = packed[part * 64 : (part + 1) * 64] * keep

    pl.semaphore_wait(barrier, 10)
    signal(ring_sems.at[0])
    for copy in leg_copies[4:]:
        copy.start()

    def legs(jp, carry):
        for jt in range(2):
            pltpu.make_async_copy(leg_hbm.at[:, 2 * jp + jt], leg.at[2 * jp + jt], leg_sem.at[2 * jp + jt]).wait()
        table = jnp.concatenate(
            [leg[2 * jp].reshape(2 * ROWS, 128), leg[2 * jp + 1].reshape(2 * ROWS, 128)], axis=1
        )
        spec[:, pl.ds(pl.multiple_of(jp * 256, 256), 256)] = jnp.dot(
            stacked[...], table, preferred_element_type=F32
        ).astype(BF16)
        return carry

    lax.fori_loop(0, 3, legs, 0)
    pl.semaphore_wait(ring_sems.at[0], 10)
    signal(ring_sems.at[1])
    lax.fori_loop(3, 4, legs, 0)

    def choose(ib, carry):
        row = pl.multiple_of(ib * 256, 256)
        outbox[pl.ds(pl.multiple_of(ib * 32, 32), 32)] = (
            lax.dot_general(
                onehot[pl.ds(row, 256), :], spec[...], (((1,), (1,)), ((), ())), preferred_element_type=F32
            )
            .reshape(32, 8, COLS)
            .astype(BF16)
        )
        return carry

    lax.fori_loop(0, 4, choose, 0)

    def send(dz, dy, dx, dc):
        target = at(dz, dy, dx, dc)
        pltpu.make_async_remote_copy(
            src_ref=outbox.at[target], dst_ref=inbox.at[me], send_sem=send_sem, recv_sem=recv_sem.at[dz],
            device_id={"blk": target}, device_id_type=MESH,
        ).start()

    def send_all(planes, axes, flip):
        count = 3 ** len(axes)

        def one(t, carry):
            offset = [0, 0, 0, flip]
            rest = t
            for axis in axes:
                offset[axis] = rest % 3 + 1
                rest = rest // 3
            for dz in planes:
                send(dz, *offset[1:])
            return carry

        if count == 1:
            one(0, 0)
        else:
            lax.fori_loop(0, count, one, 0)

    beside = 1 + 2 * (z % 2)
    across = 4 - beside
    send_all((beside, 0, across), (2,), 0)
    send_all((beside, 0, across), (1,), 0)
    send_all((beside, 0, across), (), 1)
    send_all((beside, across), (), 0)
    send_all((0,), (1, 2), 0)
    send_all((0,), (1,), 1)
    send_all((0,), (2,), 1)

    place = me % PLANE
    is_even = lax.broadcasted_iota(I32, (1, 128), 1) < FIELDS
    energy = jnp.zeros((1, 128), F32)
    for p in range(2):
        order = order_cols[pl.ds(me * 2 + p, 1), :]
        has_zero = jnp.where(order % 2 == 1, DEGREE - order, order) == 0
        for part in range(2):
            row = (p * 2 + part) * 128
            squares = jnp.zeros((128, 128), F32)
            for jb in range(8):
                values = spec[row : row + 128, jb * 128 : (jb + 1) * 128].astype(F32)
                squares = squares + values * values
            weight = jnp.where(is_even, jnp.where(has_zero, 1.0 - part, 2.0), 2.0)
            energy = energy + weight * jnp.sum(squares.T, axis=0, keepdims=True)
    e_mine[0] = energy
    e_all[z] = energy
    pl.semaphore_wait(ring_sems.at[1], 10)
    signal(ring_sems.at[2])
    for d in range(1, 4):
        pltpu.make_async_remote_copy(
            src_ref=e_mine.at[0], dst_ref=e_all.at[z], send_sem=e_sems.at[2], recv_sem=e_sems.at[3],
            device_id={"blk": at(d, 0, 0, 0)}, device_id_type=MESH,
        ).start()
    for axes, flip in (((1, 2), 0), ((1,), 1), ((2,), 1)):
        send_all((beside, across), axes, flip)
    send_all((0,), (1, 2), 1)

    pl.semaphore_wait(ring_sems.at[2], 10)
    send_all((beside, across), (1, 2), 1)
    inbox[me] = outbox[me]


    def back_of(slot):
        return slot % 2 * across * (1 - slot // 2) + slot // 2 * (beside + slot % 2 * (2 - beside))

    lane = lax.broadcasted_iota(I32, (16, 128), 1)

    def basis_step(step, carry):
        slot, sub = step // 2, step % 2
        first = (z + 4 - back_of(slot)) % 4 * 64 + sub * 32
        for p in range(2):
            order = order_cols[pl.ds(first + p, 16, stride=2), :]
            even = jnp.where((order & 1) == 1, DEGREE - order, order)
            for parity in range(2):
                m = even if parity == 0 else DEGREE - even
                cosine, sine = sincos(m * lane)
                turn_cos, turn_sin = sincos(m * 128)
                factor = jnp.where(m == 0, 1.0, 2.0)
                re, im = factor * cosine, -factor * sine
                row = pl.multiple_of(parity * COLS + slot * 128 + p * 64 + sub * 16, 16)
                for a in range(HALF // 128):
                    basis[pl.ds(row, 16), a * 128 : (a + 1) * 128] = re.astype(BF16)
                    basis[pl.ds(row + 32, 16), a * 128 : (a + 1) * 128] = im.astype(BF16)
                    re, im = re * turn_cos + im * turn_sin, im * turn_cos - re * turn_sin
        return carry

    lax.fori_loop(0, 8, basis_step, 0)

    def landed(back, count):
        pltpu.make_async_remote_copy(
            src_ref=outbox.at[pl.ds(0, count)], dst_ref=inbox.at[pl.ds(0, count)],
            send_sem=send_sem, recv_sem=recv_sem.at[back], device_id={"blk": at(0, 0, 0, 1)}, device_id_type=MESH,
        ).wait_recv()

    def build(slot, even_to, odd_to, col):
        plane = (z + 4 - back_of(slot)) % 4
        for g in range(4):
            wide[g] = inbox[pl.ds(plane * PLANE, PLANE), :, g * 128 : (g + 1) * 128].astype(F32).reshape(256, 128)
        for i in range(8):
            block = jnp.concatenate([wide[g, pl.ds(i, PLANE, stride=8), :] for g in range(4)], axis=0)
            block = block.T.astype(BF16)
            even_to[i * 64 : (i + 1) * 64, pl.ds(col, 128)] = block[:64]
            odd_to[i * 64 : (i + 1) * 64, pl.ds(col, 128)] = block[64:]

    def build_first(slot, carry):
        @pl.when(slot == 0)
        def _():
            landed(0, PLANE - 1)

        @pl.when(slot > 0)
        def _():
            landed(back_of(slot), PLANE)

        build(slot, first_x.at[0], first_x.at[1], pl.multiple_of(slot * 128, 128))
        return carry

    def sum_first(n, carry):
        cols = pl.ds(pl.multiple_of(n * 256, 256), 256)
        evens[:, cols] = jnp.dot(first_x[0], basis[:384, cols], preferred_element_type=F32)
        odds[:, cols] = jnp.dot(first_x[1], basis[COLS : COLS + 384, cols], preferred_element_type=F32)
        return carry

    told = pltpu.make_async_remote_copy(
        src_ref=e_all.at[pl.ds(0, 3)], dst_ref=e_all.at[pl.ds(0, 3)],
        send_sem=e_sems.at[2], recv_sem=e_sems.at[3], device_id={"blk": at(0, 0, 0, 1)}, device_id_type=MESH,
    )
    told.wait_send()
    told.wait_recv()
    column_sum = (e_all[0] + e_all[1]) + (e_all[2] + e_all[3])
    e_mine[1] = column_sum
    e_plane[place] = column_sum
    lax.fori_loop(0, 1, build_first, 0)

    def tell(t, carry):
        target = at(0, t // 8, (t // 2) % 4, t % 2)
        pltpu.make_async_remote_copy(
            src_ref=e_mine.at[1], dst_ref=e_plane.at[place], send_sem=e_sems.at[0], recv_sem=e_sems.at[1],
            device_id={"blk": target}, device_id_type=MESH,
        ).start()
        return carry

    lax.fori_loop(1, PLANE, tell, 0)
    for axes, flip in (((), 0), ((2,), 0), ((1,), 0), ((), 1), ((1, 2), 0), ((1,), 1), ((2,), 1), ((1, 2), 1)):
        send_all((2,), axes, flip)
    lax.fori_loop(1, 3, build_first, 0)
    lax.fori_loop(0, 8, sum_first, 0)
    told = pltpu.make_async_remote_copy(
        src_ref=e_plane.at[pl.ds(0, PLANE - 1)], dst_ref=e_plane.at[pl.ds(0, PLANE - 1)],
        send_sem=e_sems.at[0], recv_sem=e_sems.at[1], device_id={"blk": at(0, 0, 0, 1)}, device_id_type=MESH,
    )
    told.wait_send()
    told.wait_recv()
    total = e_plane[0]
    for s in range(1, PLANE):
        total = total + e_plane[s]
    energy_ref[...] = total

    landed(2, PLANE)
    build(3, even_x, odd_x, 0)
    sent = pltpu.make_async_remote_copy(
        src_ref=outbox.at[pl.ds(0, NBLK - 1)], dst_ref=inbox.at[pl.ds(0, NBLK - 1)],
        send_sem=send_sem, recv_sem=recv_sem.at[0], device_id={"blk": at(0, 0, 0, 1)}, device_id_type=MESH,
    )
    sent.wait_send()


def synthesize(energy_in, even_x, odd_x, basis, evens, odds, potential_hbm, energy_ref, tile, tile_sems):
    both = energy_in[...]
    energy_ref[...] = (both[:, :FIELDS] + both[:, FIELDS:]) * (1.0 / NLAT)
    steps = HALF // 256
    copies = []
    for n in range(steps):
        cols = slice(n * 256, (n + 1) * 256)
        even = evens[:, cols] + jnp.dot(even_x[...], basis[384:COLS, cols], preferred_element_type=F32)
        odd = odds[:, cols] + jnp.dot(odd_x[...], basis[COLS + 384 :, cols], preferred_element_type=F32)
        for half in range(2):
            tile[n, half] = (even + odd if half == 0 else even - odd).astype(BF16).reshape(8, FIELDS, 256)
            copy = pltpu.make_async_copy(
                tile.at[n, half], potential_hbm.at[:, :, pl.ds(half * HALF + n * 256, 256)], tile_sems.at[n, half]
            )
            copy.start()
            copies.append(copy)
    for copy in copies:
        copy.wait()


def shards(load_coef, legendre, slab_orders, cycle_rows):
    any_space = pl.BlockSpec(memory_space=pl.ANY)
    vmem = pl.BlockSpec(memory_space=pltpu.VMEM)
    coef = load_coef.transpose(1, 0, 2)
    table = legendre.transpose(1, 0, 2).reshape(ROWS, 2, 8, 128).transpose(0, 2, 1, 3)
    even_x, odd_x, basis, evens, odds, energy = pl.pallas_call(
        exchange,
        out_shape=(
            jax.ShapeDtypeStruct((COLS, 128), BF16),
            jax.ShapeDtypeStruct((COLS, 128), BF16),
            jax.ShapeDtypeStruct((2 * COLS, HALF), BF16),
            jax.ShapeDtypeStruct((COLS, HALF), F32),
            jax.ShapeDtypeStruct((COLS, HALF), F32),
            jax.ShapeDtypeStruct((1, 128), F32),
        ),
        in_specs=[pl.BlockSpec(memory_space=pltpu.HBM)] * 4,
        out_specs=(vmem,) * 6,
        scratch_shapes=[
            pltpu.VMEM((2, 128), I32),
            pltpu.VMEM((8, 128), I32),
            pltpu.VMEM((ROWS, 2, 128), BF16),
            pltpu.VMEM((8, ROWS, 2, 128), BF16),
            pltpu.VMEM((2, COLS, 384), BF16),
            pltpu.VMEM((COLS, 2 * ROWS), BF16),
            pltpu.VMEM((COLS, NLAT), BF16),
            pltpu.VMEM((NLAT, NLAT), BF16),
            pltpu.VMEM((NBLK, 8, COLS), BF16),
            pltpu.VMEM((NBLK, 8, COLS), BF16),
            pltpu.VMEM((4, 256, 128), F32),
            pltpu.VMEM((256, 128), I32),
            pltpu.VMEM((2, 1, 128), F32),
            pltpu.VMEM((PLANE, 1, 128), F32),
            pltpu.VMEM((4, 1, 128), F32),
            pltpu.SemaphoreType.DMA((2,)),
            pltpu.SemaphoreType.DMA,
            pltpu.SemaphoreType.DMA((8,)),
            pltpu.SemaphoreType.DMA,
            pltpu.SemaphoreType.DMA((4,)),
            pltpu.SemaphoreType.DMA((4,)),
            pltpu.SemaphoreType.REGULAR((3,)),
        ],
        compiler_params=pltpu.CompilerParams(
            collective_id=0, has_side_effects=True, vmem_limit_bytes=36 * 1024 * 1024
        ),
        name="exchange",
    )(*[pltpu.with_memory_space_constraint(a, pltpu.HBM) for a in (slab_orders.reshape(2, 128), cycle_rows.reshape(8, 128), coef, table)])
    potential, energy = pl.pallas_call(
        synthesize,
        out_shape=(
            jax.ShapeDtypeStruct((8, FIELDS, NLON), BF16),
            jax.ShapeDtypeStruct((1, FIELDS), F32),
        ),
        in_specs=[vmem] * 6,
        out_specs=(any_space, vmem),
        scratch_shapes=[
            pltpu.VMEM((8, 2, 8, FIELDS, 256), BF16),
            pltpu.SemaphoreType.DMA((8, 2)),
        ],
        compiler_params=pltpu.CompilerParams(vmem_limit_bytes=20 * 1024 * 1024),
        name="synthesize",
    )(energy, even_x, odd_x, basis, evens, odds)
    return potential, energy.reshape(FIELDS)


def solution(mesh):
    in_specs = (P("blk", None, "rep"), P("blk", None, None), P(), P())
    out_specs = (P("blk", "rep", None), P("rep"))
    return jax.shard_map(shards, mesh=mesh, in_specs=in_specs, out_specs=out_specs, check_vma=False)
```

```python
import math

import jax
import jax.numpy as jnp
from jax import lax
from jax.experimental import pallas as pl
from jax.experimental.pallas import tpu as pltpu
from jax.sharding import PartitionSpec as P

BF16 = jnp.bfloat16
F32 = jnp.float32
I32 = jnp.int32
MESH = pl.DeviceIdType.MESH
NLON = 4096
HALF = NLON // 2
DEGREE = 2047
ROWS = 2049
NLAT = 1024
FIELDS = 64
NBLK = 128
PLANE = 32
COLS = 512


def sincos(phase):
    turned = (phase + 512) & 4095
    quadrant = turned >> 10
    theta = ((turned & 1023) - 512).astype(F32) * (2.0 * math.pi / NLON)
    t2 = theta * theta
    s = theta * (1.0 + t2 * (-1.0 / 6 + t2 * (1.0 / 120 + t2 * (-1.0 / 5040 + t2 * (1.0 / 362880)))))
    c = 1.0 + t2 * (-0.5 + t2 * (1.0 / 24 + t2 * (-1.0 / 720 + t2 * (1.0 / 40320))))
    odd = (quadrant & 1) == 1
    cosine = jnp.where(odd, s, c)
    sine = jnp.where(odd, c, s)
    flip_cos = ((quadrant + 1) & 2) == 2
    flip_sin = (quadrant & 2) == 2
    return jnp.where(flip_cos, -cosine, cosine), jnp.where(flip_sin, -sine, sine)


def exchange(
    orders_hbm, cycles_hbm, coef_hbm, leg_hbm,
    even_x, odd_x, basis, energy_ref,
    orders_v, cycles, coef, leg, stacked, spec, onehot, outbox, inbox, wide, order_cols, e_mine, e_plane, e_all,
    small_sems, coef_sem, leg_sem, send_sem, recv_sem, e_sems, ring_sems,
):
    me = lax.axis_index("blk")
    z, y, x, c = me // 32, (me // 8) % 4, (me // 2) % 4, me % 2

    def at(dz, dy, dx, dc):
        return (((z + dz) % 4 * 4 + (y + dy) % 4) * 4 + (x + dx) % 4) * 2 + (c + dc) % 2

    near = [(d, 0, 0, 0) for d in (1, 2, 3)] + [(0, d, 0, 0) for d in (1, 2, 3)]
    near += [(0, 0, d, 0) for d in (1, 2, 3)] + [(0, 0, 0, 1)]

    orders_copy = pltpu.make_async_copy(orders_hbm, orders_v, small_sems.at[0])
    orders_copy.start()
    cycles_copy = pltpu.make_async_copy(cycles_hbm, cycles, small_sems.at[1])
    cycles_copy.start()
    coef_copy = pltpu.make_async_copy(coef_hbm, coef, coef_sem)
    coef_copy.start()
    leg_copies = [pltpu.make_async_copy(leg_hbm.at[:, jt], leg.at[jt], leg_sem.at[jt]) for jt in range(8)]

    barrier = pltpu.get_barrier_semaphore()

    def signal(sem):
        for offset in near:
            pl.semaphore_signal(sem, inc=1, device_id={"blk": at(*offset)}, device_id_type=MESH)

    signal(barrier)

    orders_copy.wait()
    for h in range(2):
        order_cols[h * 128 : (h + 1) * 128, :] = jnp.broadcast_to(orders_v[h : h + 1, :], (128, 128)).T
    cycles_copy.wait()
    lanes = lax.broadcasted_iota(I32, (128, 128), 1)

    def pick(ib, carry):
        wanted = jnp.broadcast_to(cycles[pl.ds(ib, 1), :], (128, 128)).T
        row = pl.multiple_of(ib * 128, 128)
        for jb in range(8):
            onehot[pl.ds(row, 128), jb * 128 : (jb + 1) * 128] = jnp.where(
                wanted == lanes + jb * 128, 1.0, 0.0
            ).astype(BF16)
        return carry

    lax.fori_loop(0, 8, pick, 0)

    coef_copy.wait()
    for copy in leg_copies[:4]:
        copy.start()
    packed = coef[...].reshape(2 * ROWS, 128).T
    column = lax.broadcasted_iota(I32, (1, 2 * ROWS), 1)
    row_id, pair_id = column >> 1, column & 1
    for p in range(2):
        order = order_cols[pl.ds(me * 2 + p, 1), :][:, :1]
        lower = jnp.where(row_id < DEGREE + 1 - order, 1, 0)
        parity_of = jnp.where(pair_id == p, (lower + order + 1) & 1, 2)
        for parity in range(2):
            keep = jnp.where(parity_of == parity, 1.0, 0.0).astype(BF16)
            for part in range(2):
                row = ((p * 2 + part) * 2 + parity) * 64
                stacked[row : row + 64, :] = packed[part * 64 : (part + 1) * 64] * keep

    pl.semaphore_wait(barrier, 10)
    signal(ring_sems.at[0])
    for copy in leg_copies[4:]:
        copy.start()

    def legs(jp, carry):
        for jt in range(2):
            pltpu.make_async_copy(leg_hbm.at[:, 2 * jp + jt], leg.at[2 * jp + jt], leg_sem.at[2 * jp + jt]).wait()
        table = jnp.concatenate(
            [leg[2 * jp].reshape(2 * ROWS, 128), leg[2 * jp + 1].reshape(2 * ROWS, 128)], axis=1
        )
        spec[:, pl.ds(pl.multiple_of(jp * 256, 256), 256)] = jnp.dot(
            stacked[...], table, preferred_element_type=F32
        ).astype(BF16)
        return carry

    lax.fori_loop(0, 3, legs, 0)
    pl.semaphore_wait(ring_sems.at[0], 10)
    signal(ring_sems.at[1])
    lax.fori_loop(3, 4, legs, 0)

    def choose(ib, carry):
        row = pl.multiple_of(ib * 256, 256)
        outbox[pl.ds(pl.multiple_of(ib * 32, 32), 32)] = (
            lax.dot_general(
                onehot[pl.ds(row, 256), :], spec[...], (((1,), (1,)), ((), ())), preferred_element_type=F32
            )
            .reshape(32, 8, COLS)
            .astype(BF16)
        )
        return carry

    lax.fori_loop(0, 4, choose, 0)

    def send(dz, dy, dx, dc):
        target = at(dz, dy, dx, dc)
        pltpu.make_async_remote_copy(
            src_ref=outbox.at[target], dst_ref=inbox.at[me], send_sem=send_sem, recv_sem=recv_sem.at[dz],
            device_id={"blk": target}, device_id_type=MESH,
        ).start()

    def send_all(planes, axes, flip):
        count = 3 ** len(axes)

        def one(t, carry):
            offset = [0, 0, 0, flip]
            rest = t
            for axis in axes:
                offset[axis] = rest % 3 + 1
                rest = rest // 3
            for dz in planes:
                send(dz, *offset[1:])
            return carry

        if count == 1:
            one(0, 0)
        else:
            lax.fori_loop(0, count, one, 0)

    beside = 1 + 2 * (z % 2)
    across = 4 - beside
    send_all((2, 1, 3), (), 0)
    send_all((2, 1, 3, 0), (2,), 0)
    send_all((2, 1, 3, 0), (1,), 0)
    send_all((2, 1, 3, 0), (), 1)
    for axes, flip in (((1, 2), 0), ((1,), 1), ((2,), 1)):
        send_all((0,), axes, flip)

    place = me % PLANE
    is_even = lax.broadcasted_iota(I32, (1, 128), 1) < FIELDS
    energy = jnp.zeros((1, 128), F32)
    for p in range(2):
        order = order_cols[pl.ds(me * 2 + p, 1), :]
        has_zero = jnp.where(order % 2 == 1, DEGREE - order, order) == 0
        for part in range(2):
            row = (p * 2 + part) * 128
            squares = jnp.zeros((128, 128), F32)
            for jb in range(8):
                values = spec[row : row + 128, jb * 128 : (jb + 1) * 128].astype(F32)
                squares = squares + values * values
            weight = jnp.where(is_even, jnp.where(has_zero, 1.0 - part, 2.0), 2.0)
            energy = energy + weight * jnp.sum(squares.T, axis=0, keepdims=True)
    e_mine[0] = energy
    e_all[z] = energy
    pl.semaphore_wait(ring_sems.at[1], 10)
    signal(ring_sems.at[2])
    for d in range(1, 4):
        pltpu.make_async_remote_copy(
            src_ref=e_mine.at[0], dst_ref=e_all.at[z], send_sem=e_sems.at[2], recv_sem=e_sems.at[3],
            device_id={"blk": at(d, 0, 0, 0)}, device_id_type=MESH,
        ).start()
    for axes, flip in (((1, 2), 0), ((1,), 1), ((2,), 1)):
        send_all((2,), axes, flip)
    send_all((0,), (1, 2), 1)
    pl.semaphore_wait(ring_sems.at[2], 10)
    send_all((2,), (1, 2), 1)
    for axes, flip in (((1, 2), 0), ((1,), 1), ((2,), 1)):
        send_all((1, 3), axes, flip)
    inbox[me] = outbox[me]


    def back_of(slot):
        late = slot // 2
        return (1 - late) * 2 * slot + late * (across + slot % 2 * (beside - across))

    lane = lax.broadcasted_iota(I32, (16, 128), 1)

    def basis_step(step, carry):
        slot, sub = step // 2, step % 2
        first = (z + 4 - back_of(slot)) % 4 * 64 + sub * 32
        for p in range(2):
            order = order_cols[pl.ds(first + p, 16, stride=2), :]
            even = jnp.where((order & 1) == 1, DEGREE - order, order)
            for parity in range(2):
                m = even if parity == 0 else DEGREE - even
                cosine, sine = sincos(m * lane)
                turn_cos, turn_sin = sincos(m * 128)
                factor = jnp.where(m == 0, 1.0, 2.0)
                re, im = factor * cosine, -factor * sine
                row = pl.multiple_of(parity * COLS + slot * 128 + p * 64 + sub * 16, 16)
                for a in range(HALF // 128):
                    basis[pl.ds(row, 16), a * 128 : (a + 1) * 128] = re.astype(BF16)
                    basis[pl.ds(row + 32, 16), a * 128 : (a + 1) * 128] = im.astype(BF16)
                    re, im = re * turn_cos + im * turn_sin, im * turn_cos - re * turn_sin
        return carry

    lax.fori_loop(0, 8, basis_step, 0)

    def landed(back, count):
        pltpu.make_async_remote_copy(
            src_ref=outbox.at[pl.ds(0, count)], dst_ref=inbox.at[pl.ds(0, count)],
            send_sem=send_sem, recv_sem=recv_sem.at[back], device_id={"blk": at(0, 0, 0, 1)}, device_id_type=MESH,
        ).wait_recv()

    def build(slot, even_to, odd_to, col):
        plane = (z + 4 - back_of(slot)) % 4
        for g in range(4):
            wide[g] = inbox[pl.ds(plane * PLANE, PLANE), :, g * 128 : (g + 1) * 128].astype(F32).reshape(256, 128)
        for i in range(8):
            block = jnp.concatenate([wide[g, pl.ds(i, PLANE, stride=8), :] for g in range(4)], axis=0)
            block = block.T.astype(BF16)
            even_to[i * 64 : (i + 1) * 64, pl.ds(col, 128)] = block[:64]
            odd_to[i * 64 : (i + 1) * 64, pl.ds(col, 128)] = block[64:]

    def build_first(slot, carry):
        @pl.when(slot == 0)
        def _():
            landed(0, PLANE - 1)

        @pl.when(slot > 0)
        def _():
            landed(back_of(slot), PLANE)

        build(slot, even_x, odd_x, pl.multiple_of(slot * 128, 128))
        return carry

    told = pltpu.make_async_remote_copy(
        src_ref=e_all.at[pl.ds(0, 3)], dst_ref=e_all.at[pl.ds(0, 3)],
        send_sem=e_sems.at[2], recv_sem=e_sems.at[3], device_id={"blk": at(0, 0, 0, 1)}, device_id_type=MESH,
    )
    told.wait_send()
    told.wait_recv()
    column_sum = (e_all[0] + e_all[1]) + (e_all[2] + e_all[3])
    e_mine[1] = column_sum
    e_plane[place] = column_sum
    lax.fori_loop(0, 1, build_first, 0)

    def tell(t, carry):
        target = at(0, t // 8, (t // 2) % 4, t % 2)
        pltpu.make_async_remote_copy(
            src_ref=e_mine.at[1], dst_ref=e_plane.at[place], send_sem=e_sems.at[0], recv_sem=e_sems.at[1],
            device_id={"blk": target}, device_id_type=MESH,
        ).start()
        return carry

    lax.fori_loop(1, PLANE, tell, 0)
    send_all((1, 3), (1, 2), 1)
    lax.fori_loop(1, 3, build_first, 0)
    told = pltpu.make_async_remote_copy(
        src_ref=e_plane.at[pl.ds(0, PLANE - 1)], dst_ref=e_plane.at[pl.ds(0, PLANE - 1)],
        send_sem=e_sems.at[0], recv_sem=e_sems.at[1], device_id={"blk": at(0, 0, 0, 1)}, device_id_type=MESH,
    )
    told.wait_send()
    told.wait_recv()
    total = e_plane[0]
    for s in range(1, PLANE):
        total = total + e_plane[s]
    energy_ref[...] = total

    lax.fori_loop(3, 4, build_first, 0)
    sent = pltpu.make_async_remote_copy(
        src_ref=outbox.at[pl.ds(0, NBLK - 1)], dst_ref=inbox.at[pl.ds(0, NBLK - 1)],
        send_sem=send_sem, recv_sem=recv_sem.at[0], device_id={"blk": at(0, 0, 0, 1)}, device_id_type=MESH,
    )
    sent.wait_send()


def synthesize(energy_in, even_x, odd_x, basis, potential_hbm, energy_ref, tile, tile_sems):
    both = energy_in[...]
    energy_ref[...] = (both[:, :FIELDS] + both[:, FIELDS:]) * (1.0 / NLAT)
    steps = HALF // 256
    copies = []
    for n in range(steps):
        cols = slice(n * 256, (n + 1) * 256)
        even = jnp.dot(even_x[...], basis[:COLS, cols], preferred_element_type=F32)
        odd = jnp.dot(odd_x[...], basis[COLS:, cols], preferred_element_type=F32)
        for half in range(2):
            tile[n, half] = (even + odd if half == 0 else even - odd).astype(BF16).reshape(8, FIELDS, 256)
            copy = pltpu.make_async_copy(
                tile.at[n, half], potential_hbm.at[:, :, pl.ds(half * HALF + n * 256, 256)], tile_sems.at[n, half]
            )
            copy.start()
            copies.append(copy)
    for copy in copies:
        copy.wait()


def shards(load_coef, legendre, slab_orders, cycle_rows):
    any_space = pl.BlockSpec(memory_space=pl.ANY)
    vmem = pl.BlockSpec(memory_space=pltpu.VMEM)
    coef = load_coef.transpose(1, 0, 2)
    table = legendre.transpose(1, 0, 2).reshape(ROWS, 2, 8, 128).transpose(0, 2, 1, 3)
    even_x, odd_x, basis, energy = pl.pallas_call(
        exchange,
        out_shape=(
            jax.ShapeDtypeStruct((COLS, COLS), BF16),
            jax.ShapeDtypeStruct((COLS, COLS), BF16),
            jax.ShapeDtypeStruct((2 * COLS, HALF), BF16),
            jax.ShapeDtypeStruct((1, 128), F32),
        ),
        in_specs=[pl.BlockSpec(memory_space=pltpu.HBM)] * 4,
        out_specs=(vmem,) * 4,
        scratch_shapes=[
            pltpu.VMEM((2, 128), I32),
            pltpu.VMEM((8, 128), I32),
            pltpu.VMEM((ROWS, 2, 128), BF16),
            pltpu.VMEM((8, ROWS, 2, 128), BF16),
            pltpu.VMEM((COLS, 2 * ROWS), BF16),
            pltpu.VMEM((COLS, NLAT), BF16),
            pltpu.VMEM((NLAT, NLAT), BF16),
            pltpu.VMEM((NBLK, 8, COLS), BF16),
            pltpu.VMEM((NBLK, 8, COLS), BF16),
            pltpu.VMEM((4, 256, 128), F32),
            pltpu.VMEM((256, 128), I32),
            pltpu.VMEM((2, 1, 128), F32),
            pltpu.VMEM((PLANE, 1, 128), F32),
            pltpu.VMEM((4, 1, 128), F32),
            pltpu.SemaphoreType.DMA((2,)),
            pltpu.SemaphoreType.DMA,
            pltpu.SemaphoreType.DMA((8,)),
            pltpu.SemaphoreType.DMA,
            pltpu.SemaphoreType.DMA((4,)),
            pltpu.SemaphoreType.DMA((4,)),
            pltpu.SemaphoreType.REGULAR((3,)),
        ],
        compiler_params=pltpu.CompilerParams(
            collective_id=0, has_side_effects=True, vmem_limit_bytes=36 * 1024 * 1024
        ),
        name="exchange",
    )(*[pltpu.with_memory_space_constraint(a, pltpu.HBM) for a in (slab_orders.reshape(2, 128), cycle_rows.reshape(8, 128), coef, table)])
    potential, energy = pl.pallas_call(
        synthesize,
        out_shape=(
            jax.ShapeDtypeStruct((8, FIELDS, NLON), BF16),
            jax.ShapeDtypeStruct((1, FIELDS), F32),
        ),
        in_specs=[vmem] * 4,
        out_specs=(any_space, vmem),
        scratch_shapes=[
            pltpu.VMEM((8, 2, 8, FIELDS, 256), BF16),
            pltpu.SemaphoreType.DMA((8, 2)),
        ],
        compiler_params=pltpu.CompilerParams(vmem_limit_bytes=20 * 1024 * 1024),
        name="synthesize",
    )(energy, even_x, odd_x, basis)
    return potential, energy.reshape(FIELDS)


def solution(mesh):
    in_specs = (P("blk", None, "rep"), P("blk", None, None), P(), P())
    out_specs = (P("blk", "rep", None), P("rep"))
    return jax.shard_map(shards, mesh=mesh, in_specs=in_specs, out_specs=out_specs, check_vma=False)
```

```python
import math

import jax
import jax.numpy as jnp
from jax import lax
from jax.experimental import pallas as pl
from jax.experimental.pallas import tpu as pltpu
from jax.sharding import PartitionSpec as P

BF16 = jnp.bfloat16
F32 = jnp.float32
I32 = jnp.int32
MESH = pl.DeviceIdType.MESH
NLON = 4096
HALF = NLON // 2
DEGREE = 2047
ROWS = 2049
NLAT = 1024
FIELDS = 64
NBLK = 128
PLANE = 32
COLS = 512


def sincos(phase):
    turned = (phase + 512) & 4095
    quadrant = turned >> 10
    theta = ((turned & 1023) - 512).astype(F32) * (2.0 * math.pi / NLON)
    t2 = theta * theta
    s = theta * (1.0 + t2 * (-1.0 / 6 + t2 * (1.0 / 120 + t2 * (-1.0 / 5040 + t2 * (1.0 / 362880)))))
    c = 1.0 + t2 * (-0.5 + t2 * (1.0 / 24 + t2 * (-1.0 / 720 + t2 * (1.0 / 40320))))
    odd = (quadrant & 1) == 1
    cosine = jnp.where(odd, s, c)
    sine = jnp.where(odd, c, s)
    flip_cos = ((quadrant + 1) & 2) == 2
    flip_sin = (quadrant & 2) == 2
    return jnp.where(flip_cos, -cosine, cosine), jnp.where(flip_sin, -sine, sine)


def exchange(
    orders_hbm, cycles_hbm, coef_hbm, leg_hbm,
    even_x, odd_x, basis, energy_ref,
    orders_v, cycles, coef, leg, stacked, spec, onehot, outbox, inbox, wide, order_cols, e_mine, e_plane, e_all,
    small_sems, coef_sem, leg_sem, send_sem, recv_sem, e_sems, ring_sems,
):
    me = lax.axis_index("blk")
    z, y, x, c = me // 32, (me // 8) % 4, (me // 2) % 4, me % 2

    def at(dz, dy, dx, dc):
        return (((z + dz) % 4 * 4 + (y + dy) % 4) * 4 + (x + dx) % 4) * 2 + (c + dc) % 2

    near = [(d, 0, 0, 0) for d in (1, 2, 3)] + [(0, d, 0, 0) for d in (1, 2, 3)]
    near += [(0, 0, d, 0) for d in (1, 2, 3)] + [(0, 0, 0, 1)]

    orders_copy = pltpu.make_async_copy(orders_hbm, orders_v, small_sems.at[0])
    orders_copy.start()
    cycles_copy = pltpu.make_async_copy(cycles_hbm, cycles, small_sems.at[1])
    cycles_copy.start()
    coef_copy = pltpu.make_async_copy(coef_hbm, coef, coef_sem)
    coef_copy.start()
    leg_copies = [pltpu.make_async_copy(leg_hbm.at[:, jt], leg.at[jt], leg_sem.at[jt]) for jt in range(8)]

    barrier = pltpu.get_barrier_semaphore()

    def signal(sem):
        for offset in near:
            pl.semaphore_signal(sem, inc=1, device_id={"blk": at(*offset)}, device_id_type=MESH)

    signal(barrier)

    orders_copy.wait()
    for h in range(2):
        order_cols[h * 128 : (h + 1) * 128, :] = jnp.broadcast_to(orders_v[h : h + 1, :], (128, 128)).T
    cycles_copy.wait()
    lanes = lax.broadcasted_iota(I32, (128, 128), 1)

    def pick(ib, carry):
        wanted = jnp.broadcast_to(cycles[pl.ds(ib, 1), :], (128, 128)).T
        row = pl.multiple_of(ib * 128, 128)
        for jb in range(8):
            onehot[pl.ds(row, 128), jb * 128 : (jb + 1) * 128] = jnp.where(
                wanted == lanes + jb * 128, 1.0, 0.0
            ).astype(BF16)
        return carry

    lax.fori_loop(0, 8, pick, 0)

    coef_copy.wait()
    for copy in leg_copies[:4]:
        copy.start()
    packed = coef[...].reshape(2 * ROWS, 128).T
    column = lax.broadcasted_iota(I32, (1, 2 * ROWS), 1)
    row_id, pair_id = column >> 1, column & 1
    for p in range(2):
        order = order_cols[pl.ds(me * 2 + p, 1), :][:, :1]
        lower = jnp.where(row_id < DEGREE + 1 - order, 1, 0)
        parity_of = jnp.where(pair_id == p, (lower + order + 1) & 1, 2)
        for parity in range(2):
            keep = jnp.where(parity_of == parity, 1.0, 0.0).astype(BF16)
            for part in range(2):
                row = ((p * 2 + part) * 2 + parity) * 64
                stacked[row : row + 64, :] = packed[part * 64 : (part + 1) * 64] * keep

    pl.semaphore_wait(barrier, 10)
    signal(ring_sems.at[0])
    for copy in leg_copies[4:]:
        copy.start()

    for jp in range(4):
        leg_copies[2 * jp].wait()
        leg_copies[2 * jp + 1].wait()
        table = jnp.concatenate(
            [leg[2 * jp].reshape(2 * ROWS, 128), leg[2 * jp + 1].reshape(2 * ROWS, 128)], axis=1
        )
        spec[:, jp * 256 : (jp + 1) * 256] = jnp.dot(
            stacked[...], table, preferred_element_type=F32
        ).astype(BF16)
        if jp == 2:
            pl.semaphore_wait(ring_sems.at[0], 10)
            signal(ring_sems.at[1])
    outbox[...] = (
        lax.dot_general(onehot[...], spec[...], (((1,), (1,)), ((), ())), preferred_element_type=F32)
        .reshape(NBLK, 8, COLS)
        .astype(BF16)
    )

    def send(dz, dy, dx, dc):
        target = at(dz, dy, dx, dc)
        pltpu.make_async_remote_copy(
            src_ref=outbox.at[target], dst_ref=inbox.at[me], send_sem=send_sem, recv_sem=recv_sem.at[dz],
            device_id={"blk": target}, device_id_type=MESH,
        ).start()

    def send_all(planes, axes, flip):
        count = 3 ** len(axes)

        def one(t, carry):
            offset = [0, 0, 0, flip]
            rest = t
            for axis in axes:
                offset[axis] = rest % 3 + 1
                rest = rest // 3
            for dz in planes:
                send(dz, *offset[1:])
            return carry

        if count == 1:
            one(0, 0)
        else:
            lax.fori_loop(0, count, one, 0)

    beside = 1 + 2 * (z % 2)
    across = 4 - beside
    send_all((2, 1, 3), (), 0)
    send_all((2, 1, 3, 0), (2,), 0)
    send_all((2, 1, 3, 0), (1,), 0)
    send_all((2, 1, 3, 0), (), 1)
    for axes, flip in (((1, 2), 0), ((1,), 1), ((2,), 1)):
        send_all((0,), axes, flip)

    place = me % PLANE
    is_even = lax.broadcasted_iota(I32, (1, 128), 1) < FIELDS
    energy = jnp.zeros((1, 128), F32)
    for p in range(2):
        order = order_cols[pl.ds(me * 2 + p, 1), :]
        has_zero = jnp.where(order % 2 == 1, DEGREE - order, order) == 0
        for part in range(2):
            row = (p * 2 + part) * 128
            squares = jnp.zeros((128, 128), F32)
            for jb in range(8):
                values = spec[row : row + 128, jb * 128 : (jb + 1) * 128].astype(F32)
                squares = squares + values * values
            weight = jnp.where(is_even, jnp.where(has_zero, 1.0 - part, 2.0), 2.0)
            energy = energy + weight * jnp.sum(squares.T, axis=0, keepdims=True)
    e_mine[0] = energy
    e_all[z] = energy
    pl.semaphore_wait(ring_sems.at[1], 10)
    signal(ring_sems.at[2])
    for d in range(1, 4):
        pltpu.make_async_remote_copy(
            src_ref=e_mine.at[0], dst_ref=e_all.at[z], send_sem=e_sems.at[2], recv_sem=e_sems.at[3],
            device_id={"blk": at(d, 0, 0, 0)}, device_id_type=MESH,
        ).start()
    for axes, flip in (((1, 2), 0), ((1,), 1), ((2,), 1)):
        send_all((2,), axes, flip)
    send_all((0,), (1, 2), 1)
    pl.semaphore_wait(ring_sems.at[2], 10)
    send_all((2,), (1, 2), 1)
    for axes, flip in (((1, 2), 0), ((1,), 1), ((2,), 1)):
        send_all((1, 3), axes, flip)
    inbox[me] = outbox[me]


    def back_of(slot):
        late = slot // 2
        return (1 - late) * 2 * slot + late * (across + slot % 2 * (beside - across))

    lane = lax.broadcasted_iota(I32, (16, 128), 1)

    def basis_step(step, carry):
        slot, sub = step // 2, step % 2
        first = (z + 4 - back_of(slot)) % 4 * 64 + sub * 32
        for p in range(2):
            order = order_cols[pl.ds(first + p, 16, stride=2), :]
            even = jnp.where((order & 1) == 1, DEGREE - order, order)
            for parity in range(2):
                m = even if parity == 0 else DEGREE - even
                cosine, sine = sincos(m * lane)
                turn_cos, turn_sin = sincos(m * 128)
                factor = jnp.where(m == 0, 1.0, 2.0)
                re, im = factor * cosine, -factor * sine
                row = pl.multiple_of(parity * COLS + slot * 128 + p * 64 + sub * 16, 16)
                for a in range(HALF // 128):
                    basis[pl.ds(row, 16), a * 128 : (a + 1) * 128] = re.astype(BF16)
                    basis[pl.ds(row + 32, 16), a * 128 : (a + 1) * 128] = im.astype(BF16)
                    re, im = re * turn_cos + im * turn_sin, im * turn_cos - re * turn_sin
        return carry

    lax.fori_loop(0, 8, basis_step, 0)

    def landed(back, count):
        pltpu.make_async_remote_copy(
            src_ref=outbox.at[pl.ds(0, count)], dst_ref=inbox.at[pl.ds(0, count)],
            send_sem=send_sem, recv_sem=recv_sem.at[back], device_id={"blk": at(0, 0, 0, 1)}, device_id_type=MESH,
        ).wait_recv()

    def build(slot, even_to, odd_to, col):
        plane = (z + 4 - back_of(slot)) % 4
        for g in range(4):
            wide[g] = inbox[pl.ds(plane * PLANE, PLANE), :, g * 128 : (g + 1) * 128].astype(F32).reshape(256, 128)
        for i in range(8):
            block = jnp.concatenate([wide[g, pl.ds(i, PLANE, stride=8), :] for g in range(4)], axis=0)
            block = block.T.astype(BF16)
            even_to[i * 64 : (i + 1) * 64, pl.ds(col, 128)] = block[:64]
            odd_to[i * 64 : (i + 1) * 64, pl.ds(col, 128)] = block[64:]

    def build_first(slot, carry):
        @pl.when(slot == 0)
        def _():
            landed(0, PLANE - 1)

        @pl.when(slot > 0)
        def _():
            landed(back_of(slot), PLANE)

        build(slot, even_x, odd_x, pl.multiple_of(slot * 128, 128))
        return carry

    told = pltpu.make_async_remote_copy(
        src_ref=e_all.at[pl.ds(0, 3)], dst_ref=e_all.at[pl.ds(0, 3)],
        send_sem=e_sems.at[2], recv_sem=e_sems.at[3], device_id={"blk": at(0, 0, 0, 1)}, device_id_type=MESH,
    )
    told.wait_send()
    told.wait_recv()
    column_sum = (e_all[0] + e_all[1]) + (e_all[2] + e_all[3])
    e_mine[1] = column_sum
    e_plane[place] = column_sum
    lax.fori_loop(0, 1, build_first, 0)

    def tell(t, carry):
        target = at(0, t // 8, (t // 2) % 4, t % 2)
        pltpu.make_async_remote_copy(
            src_ref=e_mine.at[1], dst_ref=e_plane.at[place], send_sem=e_sems.at[0], recv_sem=e_sems.at[1],
            device_id={"blk": target}, device_id_type=MESH,
        ).start()
        return carry

    lax.fori_loop(1, PLANE, tell, 0)
    send_all((1, 3), (1, 2), 1)
    lax.fori_loop(1, 3, build_first, 0)
    told = pltpu.make_async_remote_copy(
        src_ref=e_plane.at[pl.ds(0, PLANE - 1)], dst_ref=e_plane.at[pl.ds(0, PLANE - 1)],
        send_sem=e_sems.at[0], recv_sem=e_sems.at[1], device_id={"blk": at(0, 0, 0, 1)}, device_id_type=MESH,
    )
    told.wait_send()
    told.wait_recv()
    total = e_plane[0]
    for s in range(1, PLANE):
        total = total + e_plane[s]
    energy_ref[...] = total

    lax.fori_loop(3, 4, build_first, 0)
    sent = pltpu.make_async_remote_copy(
        src_ref=outbox.at[pl.ds(0, NBLK - 1)], dst_ref=inbox.at[pl.ds(0, NBLK - 1)],
        send_sem=send_sem, recv_sem=recv_sem.at[0], device_id={"blk": at(0, 0, 0, 1)}, device_id_type=MESH,
    )
    sent.wait_send()


def synthesize(energy_in, even_x, odd_x, basis, potential_hbm, energy_ref, tile, tile_sems):
    both = energy_in[...]
    energy_ref[...] = (both[:, :FIELDS] + both[:, FIELDS:]) * (1.0 / NLAT)
    steps = HALF // 256
    copies = []
    for n in range(steps):
        cols = slice(n * 256, (n + 1) * 256)
        even = jnp.dot(even_x[...], basis[:COLS, cols], preferred_element_type=F32)
        odd = jnp.dot(odd_x[...], basis[COLS:, cols], preferred_element_type=F32)
        for half in range(2):
            tile[n, half] = (even + odd if half == 0 else even - odd).astype(BF16).reshape(8, FIELDS, 256)
            copy = pltpu.make_async_copy(
                tile.at[n, half], potential_hbm.at[:, :, pl.ds(half * HALF + n * 256, 256)], tile_sems.at[n, half]
            )
            copy.start()
            copies.append(copy)
    for copy in copies:
        copy.wait()


def shards(load_coef, legendre, slab_orders, cycle_rows):
    any_space = pl.BlockSpec(memory_space=pl.ANY)
    vmem = pl.BlockSpec(memory_space=pltpu.VMEM)
    coef = load_coef.transpose(1, 0, 2)
    table = legendre.transpose(1, 0, 2).reshape(ROWS, 2, 8, 128).transpose(0, 2, 1, 3)
    even_x, odd_x, basis, energy = pl.pallas_call(
        exchange,
        out_shape=(
            jax.ShapeDtypeStruct((COLS, COLS), BF16),
            jax.ShapeDtypeStruct((COLS, COLS), BF16),
            jax.ShapeDtypeStruct((2 * COLS, HALF), BF16),
            jax.ShapeDtypeStruct((1, 128), F32),
        ),
        in_specs=[pl.BlockSpec(memory_space=pltpu.HBM)] * 4,
        out_specs=(vmem,) * 4,
        scratch_shapes=[
            pltpu.VMEM((2, 128), I32),
            pltpu.VMEM((8, 128), I32),
            pltpu.VMEM((ROWS, 2, 128), BF16),
            pltpu.VMEM((8, ROWS, 2, 128), BF16),
            pltpu.VMEM((COLS, 2 * ROWS), BF16),
            pltpu.VMEM((COLS, NLAT), BF16),
            pltpu.VMEM((NLAT, NLAT), BF16),
            pltpu.VMEM((NBLK, 8, COLS), BF16),
            pltpu.VMEM((NBLK, 8, COLS), BF16),
            pltpu.VMEM((4, 256, 128), F32),
            pltpu.VMEM((256, 128), I32),
            pltpu.VMEM((2, 1, 128), F32),
            pltpu.VMEM((PLANE, 1, 128), F32),
            pltpu.VMEM((4, 1, 128), F32),
            pltpu.SemaphoreType.DMA((2,)),
            pltpu.SemaphoreType.DMA,
            pltpu.SemaphoreType.DMA((8,)),
            pltpu.SemaphoreType.DMA,
            pltpu.SemaphoreType.DMA((4,)),
            pltpu.SemaphoreType.DMA((4,)),
            pltpu.SemaphoreType.REGULAR((3,)),
        ],
        compiler_params=pltpu.CompilerParams(
            collective_id=0, has_side_effects=True, vmem_limit_bytes=36 * 1024 * 1024
        ),
        name="exchange",
    )(*[pltpu.with_memory_space_constraint(a, pltpu.HBM) for a in (slab_orders.reshape(2, 128), cycle_rows.reshape(8, 128), coef, table)])
    potential, energy = pl.pallas_call(
        synthesize,
        out_shape=(
            jax.ShapeDtypeStruct((8, FIELDS, NLON), BF16),
            jax.ShapeDtypeStruct((1, FIELDS), F32),
        ),
        in_specs=[vmem] * 4,
        out_specs=(any_space, vmem),
        scratch_shapes=[
            pltpu.VMEM((8, 2, 8, FIELDS, 256), BF16),
            pltpu.SemaphoreType.DMA((8, 2)),
        ],
        compiler_params=pltpu.CompilerParams(vmem_limit_bytes=20 * 1024 * 1024),
        name="synthesize",
    )(energy, even_x, odd_x, basis)
    return potential, energy.reshape(FIELDS)


def solution(mesh):
    in_specs = (P("blk", None, "rep"), P("blk", None, None), P(), P())
    out_specs = (P("blk", "rep", None), P("rep"))
    return jax.shard_map(shards, mesh=mesh, in_specs=in_specs, out_specs=out_specs, check_vma=False)
```

```python
import math

import jax
import jax.numpy as jnp
from jax import lax
from jax.experimental import pallas as pl
from jax.experimental.pallas import tpu as pltpu
from jax.sharding import PartitionSpec as P

BF16 = jnp.bfloat16
F32 = jnp.float32
I32 = jnp.int32
MESH = pl.DeviceIdType.MESH
NLON = 4096
HALF = NLON // 2
DEGREE = 2047
ROWS = 2049
NLAT = 1024
FIELDS = 64
NBLK = 128
PLANE = 32
COLS = 512


def sincos(phase):
    turned = (phase + 512) & 4095
    quadrant = turned >> 10
    theta = ((turned & 1023) - 512).astype(F32) * (2.0 * math.pi / NLON)
    t2 = theta * theta
    s = theta * (1.0 + t2 * (-1.0 / 6 + t2 * (1.0 / 120 + t2 * (-1.0 / 5040 + t2 * (1.0 / 362880)))))
    c = 1.0 + t2 * (-0.5 + t2 * (1.0 / 24 + t2 * (-1.0 / 720 + t2 * (1.0 / 40320))))
    odd = (quadrant & 1) == 1
    cosine = jnp.where(odd, s, c)
    sine = jnp.where(odd, c, s)
    flip_cos = ((quadrant + 1) & 2) == 2
    flip_sin = (quadrant & 2) == 2
    return jnp.where(flip_cos, -cosine, cosine), jnp.where(flip_sin, -sine, sine)


def exchange(
    orders_hbm, cycles_hbm, coef_hbm, leg_hbm,
    even_x, odd_x, basis, energy_ref,
    orders_v, cycles, coef, leg, stacked, spec, onehot, outbox, inbox, wide, order_cols, e_mine, e_plane, e_all,
    small_sems, coef_sem, leg_sem, send_sem, recv_sem, e_sems, ring_sems,
):
    me = lax.axis_index("blk")
    z, y, x, c = me // 32, (me // 8) % 4, (me // 2) % 4, me % 2

    def at(dz, dy, dx, dc):
        return (((z + dz) % 4 * 4 + (y + dy) % 4) * 4 + (x + dx) % 4) * 2 + (c + dc) % 2

    near = [(d, 0, 0, 0) for d in (1, 2, 3)] + [(0, d, 0, 0) for d in (1, 2, 3)]
    near += [(0, 0, d, 0) for d in (1, 2, 3)] + [(0, 0, 0, 1)]

    orders_copy = pltpu.make_async_copy(orders_hbm, orders_v, small_sems.at[0])
    orders_copy.start()
    cycles_copy = pltpu.make_async_copy(cycles_hbm, cycles, small_sems.at[1])
    cycles_copy.start()
    coef_copy = pltpu.make_async_copy(coef_hbm, coef, coef_sem)
    coef_copy.start()
    leg_copies = [pltpu.make_async_copy(leg_hbm.at[:, jt], leg.at[jt], leg_sem.at[jt]) for jt in range(8)]

    barrier = pltpu.get_barrier_semaphore()

    def signal(sem):
        for offset in near:
            pl.semaphore_signal(sem, inc=1, device_id={"blk": at(*offset)}, device_id_type=MESH)

    signal(barrier)

    orders_copy.wait()
    for h in range(2):
        order_cols[h * 128 : (h + 1) * 128, :] = jnp.broadcast_to(orders_v[h : h + 1, :], (128, 128)).T
    cycles_copy.wait()
    lanes = lax.broadcasted_iota(I32, (128, 128), 1)

    def pick(ib, carry):
        wanted = jnp.broadcast_to(cycles[pl.ds(ib, 1), :], (128, 128)).T
        row = pl.multiple_of(ib * 128, 128)
        for jb in range(8):
            onehot[pl.ds(row, 128), jb * 128 : (jb + 1) * 128] = jnp.where(
                wanted == lanes + jb * 128, 1.0, 0.0
            ).astype(BF16)
        return carry

    lax.fori_loop(0, 8, pick, 0)

    coef_copy.wait()
    for copy in leg_copies[:4]:
        copy.start()
    def stack(columns, first, count):
        packed = coef[pl.ds(first, count)].reshape(2 * count, 128).T
        column = lax.broadcasted_iota(I32, (1, 2 * count), 1)
        row_id, pair_id = first + (column >> 1), column & 1
        for p in range(2):
            order = order_cols[pl.ds(me * 2 + p, 1), :][:, :1]
            lower = jnp.where(row_id < DEGREE + 1 - order, 1, 0)
            parity_of = jnp.where(pair_id == p, (lower + order + 1) & 1, 2)
            for parity in range(2):
                keep = jnp.where(parity_of == parity, 1.0, 0.0).astype(BF16)
                for part in range(2):
                    row = ((p * 2 + part) * 2 + parity) * 64
                    stacked[row : row + 64, columns] = packed[part * 64 : (part + 1) * 64] * keep

    def stack_step(k, carry):
        stack(pl.ds(pl.multiple_of(k * 1024, 1024), 1024), k * 512, 512)
        return carry

    lax.fori_loop(0, 4, stack_step, 0)
    stack(slice(2 * ROWS - 2, 2 * ROWS), ROWS - 1, 1)

    pl.semaphore_wait(barrier, 10)
    signal(ring_sems.at[0])
    for copy in leg_copies[4:]:
        copy.start()

    def legs(jp, carry):
        for jt in range(2):
            pltpu.make_async_copy(leg_hbm.at[:, 2 * jp + jt], leg.at[2 * jp + jt], leg_sem.at[2 * jp + jt]).wait()
        table = jnp.concatenate(
            [leg[2 * jp].reshape(2 * ROWS, 128), leg[2 * jp + 1].reshape(2 * ROWS, 128)], axis=1
        )
        spec[:, pl.ds(pl.multiple_of(jp * 256, 256), 256)] = jnp.dot(
            stacked[...], table, preferred_element_type=F32
        ).astype(BF16)
        return carry

    lax.fori_loop(0, 3, legs, 0)
    pl.semaphore_wait(ring_sems.at[0], 10)
    signal(ring_sems.at[1])
    lax.fori_loop(3, 4, legs, 0)

    def choose(ib, carry):
        row = pl.multiple_of(ib * 256, 256)
        outbox[pl.ds(pl.multiple_of(ib * 32, 32), 32)] = (
            lax.dot_general(
                onehot[pl.ds(row, 256), :], spec[...], (((1,), (1,)), ((), ())), preferred_element_type=F32
            )
            .reshape(32, 8, COLS)
            .astype(BF16)
        )
        return carry

    lax.fori_loop(0, 4, choose, 0)

    def send(dz, dy, dx, dc):
        target = at(dz, dy, dx, dc)
        pltpu.make_async_remote_copy(
            src_ref=outbox.at[target], dst_ref=inbox.at[me], send_sem=send_sem, recv_sem=recv_sem.at[dz],
            device_id={"blk": target}, device_id_type=MESH,
        ).start()

    def send_all(planes, axes, flip):
        count = 3 ** len(axes)

        def one(t, carry):
            offset = [0, 0, 0, flip]
            rest = t
            for axis in axes:
                offset[axis] = rest % 3 + 1
                rest = rest // 3
            for dz in planes:
                send(dz, *offset[1:])
            return carry

        if count == 1:
            one(0, 0)
        else:
            lax.fori_loop(0, count, one, 0)

    beside = 1 + 2 * (z % 2)
    across = 4 - beside
    send_all((2, 1, 3), (), 0)
    send_all((2, 1, 3, 0), (2,), 0)
    send_all((2, 1, 3, 0), (1,), 0)
    send_all((2, 1, 3, 0), (), 1)
    for axes, flip in (((1, 2), 0), ((1,), 1), ((2,), 1)):
        send_all((0,), axes, flip)

    place = me % PLANE
    is_even = lax.broadcasted_iota(I32, (1, 128), 1) < FIELDS
    energy = jnp.zeros((1, 128), F32)
    for p in range(2):
        order = order_cols[pl.ds(me * 2 + p, 1), :]
        has_zero = jnp.where(order % 2 == 1, DEGREE - order, order) == 0
        for part in range(2):
            row = (p * 2 + part) * 128
            squares = jnp.zeros((128, 128), F32)
            for jb in range(8):
                values = spec[row : row + 128, jb * 128 : (jb + 1) * 128].astype(F32)
                squares = squares + values * values
            weight = jnp.where(is_even, jnp.where(has_zero, 1.0 - part, 2.0), 2.0)
            energy = energy + weight * jnp.sum(squares.T, axis=0, keepdims=True)
    e_mine[0] = energy
    e_all[z] = energy
    pl.semaphore_wait(ring_sems.at[1], 10)
    signal(ring_sems.at[2])
    for d in range(1, 4):
        pltpu.make_async_remote_copy(
            src_ref=e_mine.at[0], dst_ref=e_all.at[z], send_sem=e_sems.at[2], recv_sem=e_sems.at[3],
            device_id={"blk": at(d, 0, 0, 0)}, device_id_type=MESH,
        ).start()
    for axes, flip in (((1, 2), 0), ((1,), 1), ((2,), 1)):
        send_all((2,), axes, flip)
    send_all((0,), (1, 2), 1)
    pl.semaphore_wait(ring_sems.at[2], 10)
    send_all((2,), (1, 2), 1)
    for axes, flip in (((1, 2), 0), ((1,), 1), ((2,), 1)):
        send_all((1, 3), axes, flip)
    inbox[me] = outbox[me]


    def back_of(slot):
        late = slot // 2
        return (1 - late) * 2 * slot + late * (across + slot % 2 * (beside - across))

    lane = lax.broadcasted_iota(I32, (16, 128), 1)

    def basis_step(step, carry):
        slot, sub = step // 2, step % 2
        first = (z + 4 - back_of(slot)) % 4 * 64 + sub * 32
        for p in range(2):
            order = order_cols[pl.ds(first + p, 16, stride=2), :]
            even = jnp.where((order & 1) == 1, DEGREE - order, order)
            for parity in range(2):
                m = even if parity == 0 else DEGREE - even
                cosine, sine = sincos(m * lane)
                turn_cos, turn_sin = sincos(m * 128)
                factor = jnp.where(m == 0, 1.0, 2.0)
                re, im = factor * cosine, -factor * sine
                row = pl.multiple_of(parity * COLS + slot * 128 + p * 64 + sub * 16, 16)
                for a in range(HALF // 128):
                    basis[pl.ds(row, 16), a * 128 : (a + 1) * 128] = re.astype(BF16)
                    basis[pl.ds(row + 32, 16), a * 128 : (a + 1) * 128] = im.astype(BF16)
                    re, im = re * turn_cos + im * turn_sin, im * turn_cos - re * turn_sin
        return carry

    lax.fori_loop(0, 8, basis_step, 0)

    def landed(back, count):
        pltpu.make_async_remote_copy(
            src_ref=outbox.at[pl.ds(0, count)], dst_ref=inbox.at[pl.ds(0, count)],
            send_sem=send_sem, recv_sem=recv_sem.at[back], device_id={"blk": at(0, 0, 0, 1)}, device_id_type=MESH,
        ).wait_recv()

    def build(slot, even_to, odd_to, col):
        plane = (z + 4 - back_of(slot)) % 4
        for g in range(4):
            wide[g] = inbox[pl.ds(plane * PLANE, PLANE), :, g * 128 : (g + 1) * 128].astype(F32).reshape(256, 128)
        for i in range(8):
            block = jnp.concatenate([wide[g, pl.ds(i, PLANE, stride=8), :] for g in range(4)], axis=0)
            block = block.T.astype(BF16)
            even_to[i * 64 : (i + 1) * 64, pl.ds(col, 128)] = block[:64]
            odd_to[i * 64 : (i + 1) * 64, pl.ds(col, 128)] = block[64:]

    def build_first(slot, carry):
        @pl.when(slot == 0)
        def _():
            landed(0, PLANE - 1)

        @pl.when(slot > 0)
        def _():
            landed(back_of(slot), PLANE)

        build(slot, even_x, odd_x, pl.multiple_of(slot * 128, 128))
        return carry

    told = pltpu.make_async_remote_copy(
        src_ref=e_all.at[pl.ds(0, 3)], dst_ref=e_all.at[pl.ds(0, 3)],
        send_sem=e_sems.at[2], recv_sem=e_sems.at[3], device_id={"blk": at(0, 0, 0, 1)}, device_id_type=MESH,
    )
    told.wait_send()
    told.wait_recv()
    column_sum = (e_all[0] + e_all[1]) + (e_all[2] + e_all[3])
    e_mine[1] = column_sum
    e_plane[place] = column_sum
    lax.fori_loop(0, 1, build_first, 0)

    def tell(t, carry):
        target = at(0, t // 8, (t // 2) % 4, t % 2)
        pltpu.make_async_remote_copy(
            src_ref=e_mine.at[1], dst_ref=e_plane.at[place], send_sem=e_sems.at[0], recv_sem=e_sems.at[1],
            device_id={"blk": target}, device_id_type=MESH,
        ).start()
        return carry

    lax.fori_loop(1, PLANE, tell, 0)
    send_all((1, 3), (1, 2), 1)
    lax.fori_loop(1, 3, build_first, 0)
    told = pltpu.make_async_remote_copy(
        src_ref=e_plane.at[pl.ds(0, PLANE - 1)], dst_ref=e_plane.at[pl.ds(0, PLANE - 1)],
        send_sem=e_sems.at[0], recv_sem=e_sems.at[1], device_id={"blk": at(0, 0, 0, 1)}, device_id_type=MESH,
    )
    told.wait_send()
    told.wait_recv()
    total = e_plane[0]
    for s in range(1, PLANE):
        total = total + e_plane[s]
    energy_ref[...] = total

    lax.fori_loop(3, 4, build_first, 0)
    sent = pltpu.make_async_remote_copy(
        src_ref=outbox.at[pl.ds(0, NBLK - 1)], dst_ref=inbox.at[pl.ds(0, NBLK - 1)],
        send_sem=send_sem, recv_sem=recv_sem.at[0], device_id={"blk": at(0, 0, 0, 1)}, device_id_type=MESH,
    )
    sent.wait_send()


def synthesize(energy_in, even_x, odd_x, basis, potential_hbm, energy_ref, tile, tile_sems):
    both = energy_in[...]
    energy_ref[...] = (both[:, :FIELDS] + both[:, FIELDS:]) * (1.0 / NLAT)
    steps = HALF // 256
    copies = []
    for n in range(steps):
        cols = slice(n * 256, (n + 1) * 256)
        even = jnp.dot(even_x[...], basis[:COLS, cols], preferred_element_type=F32)
        odd = jnp.dot(odd_x[...], basis[COLS:, cols], preferred_element_type=F32)
        for half in range(2):
            tile[n, half] = (even + odd if half == 0 else even - odd).astype(BF16).reshape(8, FIELDS, 256)
            copy = pltpu.make_async_copy(
                tile.at[n, half], potential_hbm.at[:, :, pl.ds(half * HALF + n * 256, 256)], tile_sems.at[n, half]
            )
            copy.start()
            copies.append(copy)
    for copy in copies:
        copy.wait()


def shards(load_coef, legendre, slab_orders, cycle_rows):
    any_space = pl.BlockSpec(memory_space=pl.ANY)
    vmem = pl.BlockSpec(memory_space=pltpu.VMEM)
    coef = load_coef.transpose(1, 0, 2)
    table = legendre.transpose(1, 0, 2).reshape(ROWS, 2, 8, 128).transpose(0, 2, 1, 3)
    even_x, odd_x, basis, energy = pl.pallas_call(
        exchange,
        out_shape=(
            jax.ShapeDtypeStruct((COLS, COLS), BF16),
            jax.ShapeDtypeStruct((COLS, COLS), BF16),
            jax.ShapeDtypeStruct((2 * COLS, HALF), BF16),
            jax.ShapeDtypeStruct((1, 128), F32),
        ),
        in_specs=[pl.BlockSpec(memory_space=pltpu.HBM)] * 4,
        out_specs=(vmem,) * 4,
        scratch_shapes=[
            pltpu.VMEM((2, 128), I32),
            pltpu.VMEM((8, 128), I32),
            pltpu.VMEM((ROWS, 2, 128), BF16),
            pltpu.VMEM((8, ROWS, 2, 128), BF16),
            pltpu.VMEM((COLS, 2 * ROWS), BF16),
            pltpu.VMEM((COLS, NLAT), BF16),
            pltpu.VMEM((NLAT, NLAT), BF16),
            pltpu.VMEM((NBLK, 8, COLS), BF16),
            pltpu.VMEM((NBLK, 8, COLS), BF16),
            pltpu.VMEM((4, 256, 128), F32),
            pltpu.VMEM((256, 128), I32),
            pltpu.VMEM((2, 1, 128), F32),
            pltpu.VMEM((PLANE, 1, 128), F32),
            pltpu.VMEM((4, 1, 128), F32),
            pltpu.SemaphoreType.DMA((2,)),
            pltpu.SemaphoreType.DMA,
            pltpu.SemaphoreType.DMA((8,)),
            pltpu.SemaphoreType.DMA,
            pltpu.SemaphoreType.DMA((4,)),
            pltpu.SemaphoreType.DMA((4,)),
            pltpu.SemaphoreType.REGULAR((3,)),
        ],
        compiler_params=pltpu.CompilerParams(
            collective_id=0, has_side_effects=True, vmem_limit_bytes=36 * 1024 * 1024
        ),
        name="exchange",
    )(*[pltpu.with_memory_space_constraint(a, pltpu.HBM) for a in (slab_orders.reshape(2, 128), cycle_rows.reshape(8, 128), coef, table)])
    potential, energy = pl.pallas_call(
        synthesize,
        out_shape=(
            jax.ShapeDtypeStruct((8, FIELDS, NLON), BF16),
            jax.ShapeDtypeStruct((1, FIELDS), F32),
        ),
        in_specs=[vmem] * 4,
        out_specs=(any_space, vmem),
        scratch_shapes=[
            pltpu.VMEM((8, 2, 8, FIELDS, 256), BF16),
            pltpu.SemaphoreType.DMA((8, 2)),
        ],
        compiler_params=pltpu.CompilerParams(vmem_limit_bytes=20 * 1024 * 1024),
        name="synthesize",
    )(energy, even_x, odd_x, basis)
    return potential, energy.reshape(FIELDS)


def solution(mesh):
    in_specs = (P("blk", None, "rep"), P("blk", None, None), P(), P())
    out_specs = (P("blk", "rep", None), P("rep"))
    return jax.shard_map(shards, mesh=mesh, in_specs=in_specs, out_specs=out_specs, check_vma=False)
```
